32 devices in a mesh: orb: 4 (over x, core), gx: 2 (over y), gyz: 4 (over z).
Axes of the slice: x: 2, y: 2, z: 4, core: 2. Of those that a mesh axis runs over, the one named last changes fastest.
Arguments:
- orbitals: float32 [2, 12, 32, 32, 128], P(None, 'orb', 'gx', 'gyz'), parts along dimension 1, may hold values from -12 to 12
- potential: float32 [32, 32, 128], P('gx', 'gyz'), may hold values from -8 to 60
Outputs:
- evolved: float32 [2, 12, 32, 32, 128], P(None, 'orb', 'gx', 'gyz'), parts along dimension 1
- residual: float32 [2, 12, 32, 32, 128], P(None, 'orb', 'gx', 'gyz'), parts along dimension 1
The draws below stay inside these ranges and needn't reach their ends.
There are 4 independent parts, one for each index of `orb`. The reference program is written for one: setup_inputs(seed, part) draws one part's arguments, and reference() takes and returns one part's arrays. A program takes and returns all parts, laid end to end along the dimension named above; an argument that names none is the same for every part. Nothing has to cross between parts.
All inputs are finite; a program needn't handle non-finite values.
Results may differ from the reference program's by a relative error of at most 0.0003.
Values sent between devices are 32-bit elements; how exact they have to be, the bound alone decides.
No kernel may reach another device: no remote copies, remote signals or barrier semaphores. Data moves between devices by JAX's collectives and lax.ppermute only.
A program may use at most 64 MiB of HBM per device.

```python
import jax
import jax.numpy as jnp

ORB = 3
NZ = 128
ITERS = 4
NX = 32
NY = 32


def draw_orbitals(key, part):
    shape = (2, ORB, NX, NY, NZ)
    ramp = 1.0 + 2.0 * jnp.arange(NX, dtype=jnp.float32) / (NX - 1)
    envelope = ramp[None, None, :, None, None]
    values = jax.random.normal(jax.random.fold_in(key, 13), shape, jnp.float32)
    return jnp.clip(values, -4.0, 4.0) * envelope


def draw_potential(key, part):
    rough = jax.random.uniform(jax.random.fold_in(key, 21), (NX, NY, NZ), jnp.float32, -8.0, 8.0)
    ramp = 40.0 * jnp.arange(NX, dtype=jnp.float32)[:, None, None] / (NX - 1)
    return rough + ramp


def setup_inputs(seed: int = 0, part: int = 0) -> dict:
    splits = jax.random.split(jax.random.key(seed), 3)
    own_keys = jax.random.split(jax.random.fold_in(splits[2], part), 3)
    return {
        "orbitals": draw_orbitals(jax.random.fold_in(jax.random.fold_in(splits[2], part), 71), part),
        "potential": draw_potential(jax.random.fold_in(splits[2], 71), part),
    }


SPACING = 0.25
HALF_STEP = 0.05
COEFF_NEAR = 4.0 / 3.0
COEFF_FAR = -1.0 / 12.0
COEFF_SELF = -2.5


def laplace_apply(padded, potential):
    extent = (padded.shape[2] - 4, padded.shape[3] - 4, padded.shape[4] - 4)

    def window(shift_x, shift_y, shift_z):
        return padded[:, :, 2 + shift_x:2 + shift_x + extent[0], 2 + shift_y:2 + shift_y + extent[1], 2 + shift_z:2 + shift_z + extent[2]]

    center = window(0, 0, 0)
    summed = (3.0 * COEFF_SELF) * center
    for offset, weight in ((1, COEFF_NEAR), (2, COEFF_FAR)):
        summed = summed + weight * (window(offset, 0, 0) + window(-offset, 0, 0) + window(0, offset, 0) + window(0, -offset, 0) + window(0, 0, offset) + window(0, 0, -offset))
    return (-0.5 / SPACING ** 2) * summed + potential * center


def hamiltonian(vector, potential):
    padded = jnp.pad(vector, ((0, 0), (0, 0), (2, 2), (2, 2), (2, 2)))
    return laplace_apply(padded, potential)


def system(vector, applied):
    return jnp.stack([vector[0] - HALF_STEP * applied[1], vector[1] + HALF_STEP * applied[0]])


def precondition(vector, potential):
    diagonal = HALF_STEP * (3.75 / SPACING ** 2 + potential)
    divisor = 1.0 + diagonal * diagonal
    return jnp.stack([(vector[0] + diagonal * vector[1]) / divisor, (vector[1] - diagonal * vector[0]) / divisor])


def braket(left, right):
    real_part = jnp.sum(left[0] * right[0] + left[1] * right[1], axis=(1, 2, 3))
    imag_part = jnp.sum(left[0] * right[1] - left[1] * right[0], axis=(1, 2, 3))
    return real_part, imag_part


def times_complex(first, second):
    return (first[0] * second[0] - first[1] * second[1], first[0] * second[1] + first[1] * second[0])


def divide_complex(first, second):
    modulus = second[0] * second[0] + second[1] * second[1]
    return ((first[0] * second[0] + first[1] * second[1]) / modulus, (first[1] * second[0] - first[0] * second[1]) / modulus)


def scale_complex(coeff, vector):
    real_coef = coeff[0][:, None, None, None]
    imag_coef = coeff[1][:, None, None, None]
    return jnp.stack([real_coef * vector[0] - imag_coef * vector[1], real_coef * vector[1] + imag_coef * vector[0]])


def reference(orbitals, potential):
    h_orbitals = hamiltonian(orbitals, potential)
    residual = jnp.stack([2.0 * HALF_STEP * h_orbitals[1], -2.0 * HALF_STEP * h_orbitals[0]])
    evolved = orbitals
    shadow = residual
    direction = residual
    rho_now = braket(shadow, residual)
    for iteration in range(ITERS):
        dir_hat = precondition(direction, potential)
        image = system(dir_hat, hamiltonian(dir_hat, potential))
        alpha_step = divide_complex(rho_now, braket(shadow, image))
        half_step = residual - scale_complex(alpha_step, image)
        half_hat = precondition(half_step, potential)
        second = system(half_hat, hamiltonian(half_hat, potential))
        cross = braket(second, half_step)
        norm_second = jnp.sum(second * second, axis=(0, 2, 3, 4))
        omega_step = (cross[0] / norm_second, cross[1] / norm_second)
        evolved = evolved + scale_complex(alpha_step, dir_hat) + scale_complex(omega_step, half_hat)
        residual = half_step - scale_complex(omega_step, second)
        if iteration + 1 < ITERS:
            rho_next = braket(shadow, residual)
            beta_step = times_complex(divide_complex(rho_next, rho_now), divide_complex(alpha_step, omega_step))
            direction = residual + scale_complex(beta_step, direction - scale_complex(omega_step, image))
            rho_now = rho_next
    return evolved, residual
```

```python
import functools

import jax
import jax.numpy as jnp
from jax import lax
from jax.experimental import pallas as pl
from jax.experimental.pallas import tpu as pltpu
from jax.sharding import PartitionSpec as P

ITERS = 4


SPACING = 0.25
HALF_STEP = 0.05
COEFF_NEAR = 4.0 / 3.0
COEFF_FAR = -1.0 / 12.0
COEFF_SELF = -2.5

RATIO = -COEFF_NEAR / COEFF_FAR
K2 = HALF_STEP * -0.5 / SPACING**2 * COEFF_FAR
DIAGONAL = -0.5 / SPACING**2 * 3.0 * COEFF_SELF
MARGIN = 8
WORKING_SET = 40 * 2**20


def with_halo(array, sides, width):
    for axis, dim in sides:
        size, length = (lax.axis_size(axis), array.shape[dim])
        up = [(i, (i + 1) % size) for i in range(size - 1)]
        down = [(j, i) for i, j in up]
        last = lax.slice_in_dim(array, length - width, length, axis=dim)
        leading = lax.slice_in_dim(array, 0, width, axis=dim)
        before = lax.ppermute(last, axis, up)
        after = lax.ppermute(leading, axis, down)
        array = jnp.concatenate([before, array, after], axis=dim)
    return array


def laplace_apply(padded, potential):
    extent = (padded.shape[2] - 4, padded.shape[3] - 4, padded.shape[4] - 4)

    def window(shift_x, shift_y, shift_z):
        return padded[
            :,
            :,
            2 + shift_x : 2 + shift_x + extent[0],
            2 + shift_y : 2 + shift_y + extent[1],
            2 + shift_z : 2 + shift_z + extent[2],
        ]

    center = window(0, 0, 0)
    summed = 3.0 * COEFF_SELF * center
    for offset, weight in ((1, COEFF_NEAR), (2, COEFF_FAR)):
        summed = summed + weight * (
            window(offset, 0, 0)
            + window(-offset, 0, 0)
            + window(0, offset, 0)
            + window(0, -offset, 0)
            + window(0, 0, offset)
            + window(0, 0, -offset)
        )
    return -0.5 / SPACING**2 * summed + potential * center


def pad_depth(vector):
    return jnp.pad(vector, ((0, 0), (0, 0), (0, 0), (0, 0), (2, 2)))


def system(vector, applied):
    return jnp.stack([vector[0] - HALF_STEP * applied[1], vector[1] + HALF_STEP * applied[0]])


def precondition(vector, potential):
    diagonal = HALF_STEP * (3.75 / SPACING**2 + potential)
    divisor = 1.0 + diagonal * diagonal
    return jnp.stack(
        [(vector[0] + diagonal * vector[1]) / divisor, (vector[1] - diagonal * vector[0]) / divisor]
    )


def braket(left, right):
    real_part = jnp.sum(left[0] * right[0] + left[1] * right[1], axis=(1, 2, 3))
    imag_part = jnp.sum(left[0] * right[1] - left[1] * right[0], axis=(1, 2, 3))
    return (real_part, imag_part)


def times_complex(first, second):
    return (
        first[0] * second[0] - first[1] * second[1],
        first[0] * second[1] + first[1] * second[0],
    )


def divide_complex(first, second):
    modulus = second[0] * second[0] + second[1] * second[1]
    return (
        (first[0] * second[0] + first[1] * second[1]) / modulus,
        (first[1] * second[0] - first[0] * second[1]) / modulus,
    )


def scale_complex(coeff, vector):
    real_coef = coeff[0][:, None, None, None]
    imag_coef = coeff[1][:, None, None, None]
    return jnp.stack(
        [
            real_coef * vector[0] - imag_coef * vector[1],
            real_coef * vector[1] + imag_coef * vector[0],
        ]
    )


def distributed(orbitals, potential):
    def apply_shallow(vector):
        padded = with_halo(vector, (("gx", 2), ("gyz", 3)), 2)
        return laplace_apply(pad_depth(padded), potential)

    h_orbitals = apply_shallow(orbitals)
    residual = jnp.stack([2.0 * HALF_STEP * h_orbitals[1], -2.0 * HALF_STEP * h_orbitals[0]])
    evolved = orbitals
    shadow = residual
    direction = residual
    rho_now = lax.psum(braket(shadow, residual), ("gx", "gyz"))
    for iteration in range(ITERS):
        dir_hat = precondition(direction, potential)
        image = system(dir_hat, apply_shallow(dir_hat))
        alpha_step = divide_complex(rho_now, lax.psum(braket(shadow, image), ("gx", "gyz")))
        half_step = residual - scale_complex(alpha_step, image)
        half_hat = precondition(half_step, potential)
        second = system(half_hat, apply_shallow(half_hat))
        cross_local = braket(second, half_step)
        norm_local = jnp.sum(second * second, axis=(0, 2, 3, 4))
        shadow_half = braket(shadow, half_step)
        shadow_second = braket(shadow, second)
        summed = lax.psum(
            (
                cross_local[0],
                cross_local[1],
                norm_local,
                shadow_half[0],
                shadow_half[1],
                shadow_second[0],
                shadow_second[1],
            ),
            ("gx", "gyz"),
        )
        cross_real, cross_imag, norm_second = (summed[0], summed[1], summed[2])
        omega_step = (cross_real / norm_second, cross_imag / norm_second)
        evolved = evolved + scale_complex(alpha_step, dir_hat) + scale_complex(omega_step, half_hat)
        residual = half_step - scale_complex(omega_step, second)
        if iteration + 1 < ITERS:
            along_second = times_complex(omega_step, (summed[5], summed[6]))
            rho_next = (summed[3] - along_second[0], summed[4] - along_second[1])
            beta_step = times_complex(
                divide_complex(rho_next, rho_now), divide_complex(alpha_step, omega_step)
            )
            direction = residual + scale_complex(
                beta_step, direction - scale_complex(omega_step, image)
            )
            rho_now = rho_next
    return (evolved, residual)


def colour(a, b, rows, columns):
    return (b + (columns // rows) * a) % columns


def neighbours(rows, columns):
    return [(0, 0)] + [(0, 1), (0, columns - 1)] + [(da, 0) for da in range(1, rows)]


def covers(rows, columns, count):
    near = neighbours(rows, columns)
    return (
        columns % rows == 0
        and count <= columns
        and all(
            sorted(colour(a + da, b + db, rows, columns) for da, db in near) == list(range(columns))
            for a in range(rows)
            for b in range(columns)
        )
    )


def complex_mul(first, second):
    return (
        first[0] * second[0] - first[1] * second[1],
        first[0] * second[1] + first[1] * second[0],
    )


def pack_kernel(rows, columns, count, offsets, orbitals_ref, potential_ref, *out_refs):
    a, b = (lax.axis_index("gx"), lax.axis_index("gyz"))
    for (da, db), out_ref in zip(offsets, out_refs):
        q = lax.rem(
            b + (columns - db) + (columns // rows) * (a + (rows - da)), columns
        )
        q = jnp.minimum(q, count - 1)
        out_ref[0] = orbitals_ref[0, q]
        out_ref[1] = orbitals_ref[1, q]
        out_ref[2] = potential_ref[...]


def total(parts):
    return jnp.sum(parts, axis=(0, 1), keepdims=True)


def fold(product):
    return jnp.sum(product.reshape(-1, 8, product.shape[-1]), axis=0)


def solve_kernel(rows, columns, offsets, near, *refs):
    n_in, n_out = (len(offsets), len(near))
    blocks, outs = (refs[:n_in], refs[n_in : n_in + n_out])
    diag, inv, padded_d, padded_h, evolved, res, shadow, direc, image, second = refs[n_in + n_out :]
    _, bx, by, nz = blocks[0].shape
    nx, ny = (bx * rows, by * columns)
    a, b = (lax.axis_index("gx"), lax.axis_index("gyz"))
    zero_edge = jnp.zeros((2, 2, ny + 2 * MARGIN, nz), jnp.float32)
    for padded in (padded_d, padded_h):
        padded[:, 0:2] = zero_edge
        padded[:, nx + 2 : nx + 4] = zero_edge
        padded[:, :, 0:MARGIN] = jnp.zeros((2, nx + 4, MARGIN, nz), jnp.float32)
        padded[:, :, ny + MARGIN : ny + 2 * MARGIN] = jnp.zeros((2, nx + 4, MARGIN, nz), jnp.float32)
    for (da, db), block in zip(offsets, blocks):
        x0 = lax.rem(a + da, rows) * bx
        y0 = pl.multiple_of(lax.rem(b + db, columns) * by, 8)
        d = HALF_STEP * (DIAGONAL + block[2])
        diag[pl.ds(x0, bx), pl.ds(y0, by), :] = d
        inv[pl.ds(x0, bx), pl.ds(y0, by), :] = K2 / (1.0 + d * d)
        for part in range(2):
            padded_d[part, pl.ds(x0 + 2, bx), pl.ds(y0 + MARGIN, by), :] = block[part]
            evolved[part, pl.ds(x0, bx), pl.ds(y0, by), :] = block[part]

    lane = lax.broadcasted_iota(jnp.int32, (ny, nz), 1)
    keep = {s: (lane >= s if s > 0 else lane < nz + s) for s in (1, -1, 2, -2)}

    def shifted(center, s):
        return jnp.where(keep[s], pltpu.roll(center, s % nz, 1), 0.0)

    def stencil(padded, part, x):
        center = padded[part, x + 2, MARGIN : MARGIN + ny, :]

        def ring(s):
            return (
                (padded[part, x + 2 + s, MARGIN : MARGIN + ny, :] + padded[part, x + 2 - s, MARGIN : MARGIN + ny, :])
                + (padded[part, x + 2, MARGIN + s : MARGIN + s + ny, :] + padded[part, x + 2, MARGIN - s : MARGIN - s + ny, :])
                + (shifted(center, s) + shifted(center, -s))
            )

        return center, ring(2) - RATIO * ring(1)

    def sums(count):
        return tuple(jnp.zeros((8, nz), jnp.float32) for _ in range(count))

    def precondition_at(re, im, x):
        d, scale = (diag[x], inv[x])
        return (re + d * im) * scale, (im - d * re) * scale

    def start(x, acc):
        d = diag[x]
        center_re, off_re = stencil(padded_d, 0, x)
        center_im, off_im = stencil(padded_d, 1, x)
        re = 2.0 * (d * center_im + K2 * off_im)
        im = -2.0 * (d * center_re + K2 * off_re)
        shadow[0, x] = re
        shadow[1, x] = im
        hat_re, hat_im = precondition_at(re, im, x)
        padded_h[0, x + 2, MARGIN : MARGIN + ny, :] = hat_re
        padded_h[1, x + 2, MARGIN : MARGIN + ny, :] = hat_im
        return (acc[0] + fold(re * re + im * im),)

    (norm,) = lax.fori_loop(0, nx, start, sums(1))
    rho = (total(norm), jnp.zeros((1, 1), jnp.float32))
    residual, direction = (shadow, shadow)
    hat, other = (padded_h, padded_d)

    for iteration in range(ITERS):

        def image_at(x, acc):
            _, off_re = stencil(hat, 0, x)
            _, off_im = stencil(hat, 1, x)
            re = direction[0, x] - off_im
            im = direction[1, x] + off_re
            image[0, x] = re
            image[1, x] = im
            s_re, s_im = (shadow[0, x], shadow[1, x])
            return (acc[0] + fold(s_re * re + s_im * im), acc[1] + fold(s_re * im - s_im * re))

        acc = lax.fori_loop(0, nx, image_at, sums(2))
        sigma = (total(acc[0]), total(acc[1]))
        alpha = divide_complex(rho, sigma)
        along = complex_mul(alpha, sigma)
        shadow_half = (rho[0] - along[0], rho[1] - along[1])

        def half_at(x, carry):
            i_re, i_im = (image[0, x], image[1, x])
            re = residual[0, x] - (alpha[0] * i_re - alpha[1] * i_im)
            im = residual[1, x] - (alpha[0] * i_im + alpha[1] * i_re)
            res[0, x] = re
            res[1, x] = im
            hat_re, hat_im = precondition_at(re, im, x)
            other[0, x + 2, MARGIN : MARGIN + ny, :] = hat_re
            other[1, x + 2, MARGIN : MARGIN + ny, :] = hat_im
            return carry

        lax.fori_loop(0, nx, half_at, 0)

        def second_at(x, acc):
            _, off_re = stencil(other, 0, x)
            _, off_im = stencil(other, 1, x)
            h_re, h_im = (res[0, x], res[1, x])
            re = h_re - off_im
            im = h_im + off_re
            second[0, x] = re
            second[1, x] = im
            s_re, s_im = (shadow[0, x], shadow[1, x])
            return (
                acc[0] + fold(re * h_re + im * h_im),
                acc[1] + fold(re * h_im - im * h_re),
                acc[2] + fold(re * re + im * im),
                acc[3] + fold(s_re * re + s_im * im),
                acc[4] + fold(s_re * im - s_im * re),
            )

        acc = lax.fori_loop(0, nx, second_at, sums(5))
        cross_re, cross_im, norm, ss_re, ss_im = [total(part) for part in acc]
        omega = (cross_re / norm, cross_im / norm)
        alpha_hat = (alpha[0] * (1.0 / K2), alpha[1] * (1.0 / K2))
        omega_hat = (omega[0] * (1.0 / K2), omega[1] * (1.0 / K2))

        def step_evolved(base, at_d, at_h):
            along_d = complex_mul(alpha_hat, at_d)
            along_h = complex_mul(omega_hat, at_h)
            return (base[0] + (along_d[0] + along_h[0]), base[1] + (along_d[1] + along_h[1]))

        if iteration + 1 < ITERS:
            moved = complex_mul(omega, (ss_re, ss_im))
            rho_next = (shadow_half[0] - moved[0], shadow_half[1] - moved[1])
            beta = complex_mul(divide_complex(rho_next, rho), divide_complex(alpha, omega))
            beta_omega = complex_mul(beta, omega)
            rho = rho_next

            def update_at(x, carry):
                at_d = (hat[0, x + 2, MARGIN : MARGIN + ny, :], hat[1, x + 2, MARGIN : MARGIN + ny, :])
                at_h = (other[0, x + 2, MARGIN : MARGIN + ny, :], other[1, x + 2, MARGIN : MARGIN + ny, :])
                e = step_evolved((evolved[0, x], evolved[1, x]), at_d, at_h)
                evolved[0, x] = e[0]
                evolved[1, x] = e[1]
                w = complex_mul(omega, (second[0, x], second[1, x]))
                r_re = res[0, x] - w[0]
                r_im = res[1, x] - w[1]
                res[0, x] = r_re
                res[1, x] = r_im
                p = complex_mul(beta, (direction[0, x], direction[1, x]))
                v = complex_mul(beta_omega, (image[0, x], image[1, x]))
                p_re = r_re + (p[0] - v[0])
                p_im = r_im + (p[1] - v[1])
                direc[0, x] = p_re
                direc[1, x] = p_im
                hat_re, hat_im = precondition_at(p_re, p_im, x)
                hat[0, x + 2, MARGIN : MARGIN + ny, :] = hat_re
                hat[1, x + 2, MARGIN : MARGIN + ny, :] = hat_im
                return carry

            lax.fori_loop(0, nx, update_at, 0)
            residual, direction = (res, direc)
        else:
            for (da, db), out in zip(near, outs):
                x0 = lax.rem(a + da, rows) * bx
                y0 = pl.multiple_of(lax.rem(b + db, columns) * by, 8)

                def finish_at(i, carry):
                    x, y = (x0 + i, pl.ds(y0, by))
                    yp = pl.ds(y0 + MARGIN, by)
                    at_d = (hat[0, x + 2, yp, :], hat[1, x + 2, yp, :])
                    at_h = (other[0, x + 2, yp, :], other[1, x + 2, yp, :])
                    e = step_evolved((evolved[0, x, y, :], evolved[1, x, y, :]), at_d, at_h)
                    w = complex_mul(omega, (second[0, x, y, :], second[1, x, y, :]))
                    out[0, i] = e[0]
                    out[1, i] = e[1]
                    out[2, i] = res[0, x, y, :] - w[0]
                    out[3, i] = res[1, x, y, :] - w[1]
                    return carry

                lax.fori_loop(0, bx, finish_at, 0)


def unpack_kernel(rows, columns, count, near, *refs):
    blocks, (evolved_ref, residual_ref) = (refs[: len(near)], refs[len(near) :])
    a, b = (lax.axis_index("gx"), lax.axis_index("gyz"))
    for (da, db), block in zip(near, blocks):
        q = lax.rem(b + (columns - db) + (columns // rows) * (a + (rows - da)), columns)

        @pl.when(q < count)
        def _():
            for part in range(2):
                evolved_ref[part, q] = block[part]
                residual_ref[part, q] = block[2 + part]


VMEM_SPEC = pl.BlockSpec(memory_space=pltpu.VMEM)


def gathered(mesh_shape, orbitals, potential):
    groups, rows, columns = (mesh_shape["orb"], mesh_shape["gx"], mesh_shape["gyz"])
    _, count, bx, by, nz = orbitals.shape
    nx, ny = (bx * rows, by * columns)
    axes = ("orb", "gx", "gyz")
    offsets = [(da, db) for da in range(rows) for db in range(columns)]
    near = neighbours(rows, columns)
    places = [(g, a, b) for g in range(groups) for a in range(rows) for b in range(columns)]

    def linear(g, a, b):
        return (g * rows + a % rows) * columns + b % columns

    def shape(*dims):
        return jax.ShapeDtypeStruct(dims, jnp.float32)

    messages = pl.pallas_call(
        functools.partial(pack_kernel, rows, columns, count, offsets),
        out_shape=[shape(3, bx, by, nz)] * len(offsets),
        in_specs=[VMEM_SPEC] * 2,
        out_specs=[VMEM_SPEC] * len(offsets),
        name="pack",
    )(orbitals, potential)
    blocks = []
    for (da, db), message in zip(offsets, messages):
        if (da, db) == (0, 0):
            blocks.append(message)
            continue
        pairs = [
            (linear(g, a + da, b + db), linear(g, a, b))
            for g, a, b in places
            if colour(a, b, rows, columns) < count
        ]
        blocks.append(lax.ppermute(message, axes, pairs))
    field = pltpu.VMEM((2, nx, ny, nz), jnp.float32)
    padded = pltpu.VMEM((2, nx + 4, ny + 2 * MARGIN, nz), jnp.float32)
    scalar_field = pltpu.VMEM((nx, ny, nz), jnp.float32)
    pieces = pl.pallas_call(
        functools.partial(solve_kernel, rows, columns, offsets, near),
        out_shape=[shape(4, bx, by, nz)] * len(near),
        in_specs=[VMEM_SPEC] * len(blocks),
        out_specs=[VMEM_SPEC] * len(near),
        scratch_shapes=[scalar_field] * 2 + [padded] * 2 + [field] * 6,
        name="solve",
    )(*blocks)
    arrived = []
    for (da, db), piece in zip(near, pieces):
        if (da, db) == (0, 0):
            arrived.append(piece)
            continue
        pairs = [
            (linear(g, a, b), linear(g, a + da, b + db))
            for g, a, b in places
            if colour(a, b, rows, columns) < count
        ]
        arrived.append(lax.ppermute(piece, axes, pairs))
    return pl.pallas_call(
        functools.partial(unpack_kernel, rows, columns, count, near),
        out_shape=[shape(*orbitals.shape)] * 2,
        in_specs=[VMEM_SPEC] * len(near),
        out_specs=[VMEM_SPEC] * 2,
        name="unpack",
    )(*arrived)


def solution(mesh):
    mesh_shape = dict(mesh.shape)

    def shards(orbitals, potential):
        _, count, bx, by, nz = orbitals.shape
        rows, columns = (mesh_shape["gx"], mesh_shape["gyz"])
        fields = 24 * 4 * (bx * rows + 4) * (by * columns + 2 * MARGIN) * nz
        fits = fields <= WORKING_SET and by % 8 == 0 and nz % 128 == 0
        if fits and covers(rows, columns, count):
            return tuple(gathered(mesh_shape, orbitals, potential))
        return distributed(orbitals, potential)

    return jax.shard_map(
        shards,
        mesh=mesh,
        in_specs=(P(None, "orb", "gx", "gyz", None), P("gx", "gyz", None)),
        out_specs=(P(None, "orb", "gx", "gyz", None), P(None, "orb", "gx", "gyz", None)),
        check_vma=False,
    )
```

```python
import functools

import jax
import jax.numpy as jnp
from jax import lax
from jax.experimental import pallas as pl
from jax.experimental.pallas import tpu as pltpu
from jax.sharding import PartitionSpec as P

ITERS = 4


SPACING = 0.25
HALF_STEP = 0.05
COEFF_NEAR = 4.0 / 3.0
COEFF_FAR = -1.0 / 12.0
COEFF_SELF = -2.5

RATIO = -COEFF_NEAR / COEFF_FAR
K2 = HALF_STEP * -0.5 / SPACING**2 * COEFF_FAR
DIAGONAL = -0.5 / SPACING**2 * 3.0 * COEFF_SELF
MARGIN = 8
WORKING_SET = 40 * 2**20


def with_halo(array, sides, width):
    for axis, dim in sides:
        size, length = (lax.axis_size(axis), array.shape[dim])
        up = [(i, (i + 1) % size) for i in range(size - 1)]
        down = [(j, i) for i, j in up]
        last = lax.slice_in_dim(array, length - width, length, axis=dim)
        leading = lax.slice_in_dim(array, 0, width, axis=dim)
        before = lax.ppermute(last, axis, up)
        after = lax.ppermute(leading, axis, down)
        array = jnp.concatenate([before, array, after], axis=dim)
    return array


def laplace_apply(padded, potential):
    extent = (padded.shape[2] - 4, padded.shape[3] - 4, padded.shape[4] - 4)

    def window(shift_x, shift_y, shift_z):
        return padded[
            :,
            :,
            2 + shift_x : 2 + shift_x + extent[0],
            2 + shift_y : 2 + shift_y + extent[1],
            2 + shift_z : 2 + shift_z + extent[2],
        ]

    center = window(0, 0, 0)
    summed = 3.0 * COEFF_SELF * center
    for offset, weight in ((1, COEFF_NEAR), (2, COEFF_FAR)):
        summed = summed + weight * (
            window(offset, 0, 0)
            + window(-offset, 0, 0)
            + window(0, offset, 0)
            + window(0, -offset, 0)
            + window(0, 0, offset)
            + window(0, 0, -offset)
        )
    return -0.5 / SPACING**2 * summed + potential * center


def pad_depth(vector):
    return jnp.pad(vector, ((0, 0), (0, 0), (0, 0), (0, 0), (2, 2)))


def system(vector, applied):
    return jnp.stack([vector[0] - HALF_STEP * applied[1], vector[1] + HALF_STEP * applied[0]])


def precondition(vector, potential):
    diagonal = HALF_STEP * (3.75 / SPACING**2 + potential)
    divisor = 1.0 + diagonal * diagonal
    return jnp.stack(
        [(vector[0] + diagonal * vector[1]) / divisor, (vector[1] - diagonal * vector[0]) / divisor]
    )


def braket(left, right):
    real_part = jnp.sum(left[0] * right[0] + left[1] * right[1], axis=(1, 2, 3))
    imag_part = jnp.sum(left[0] * right[1] - left[1] * right[0], axis=(1, 2, 3))
    return (real_part, imag_part)


def times_complex(first, second):
    return (
        first[0] * second[0] - first[1] * second[1],
        first[0] * second[1] + first[1] * second[0],
    )


def divide_complex(first, second):
    modulus = second[0] * second[0] + second[1] * second[1]
    return (
        (first[0] * second[0] + first[1] * second[1]) / modulus,
        (first[1] * second[0] - first[0] * second[1]) / modulus,
    )


def scale_complex(coeff, vector):
    real_coef = coeff[0][:, None, None, None]
    imag_coef = coeff[1][:, None, None, None]
    return jnp.stack(
        [
            real_coef * vector[0] - imag_coef * vector[1],
            real_coef * vector[1] + imag_coef * vector[0],
        ]
    )


def distributed(orbitals, potential):
    def apply_shallow(vector):
        padded = with_halo(vector, (("gx", 2), ("gyz", 3)), 2)
        return laplace_apply(pad_depth(padded), potential)

    h_orbitals = apply_shallow(orbitals)
    residual = jnp.stack([2.0 * HALF_STEP * h_orbitals[1], -2.0 * HALF_STEP * h_orbitals[0]])
    evolved = orbitals
    shadow = residual
    direction = residual
    rho_now = lax.psum(braket(shadow, residual), ("gx", "gyz"))
    for iteration in range(ITERS):
        dir_hat = precondition(direction, potential)
        image = system(dir_hat, apply_shallow(dir_hat))
        alpha_step = divide_complex(rho_now, lax.psum(braket(shadow, image), ("gx", "gyz")))
        half_step = residual - scale_complex(alpha_step, image)
        half_hat = precondition(half_step, potential)
        second = system(half_hat, apply_shallow(half_hat))
        cross_local = braket(second, half_step)
        norm_local = jnp.sum(second * second, axis=(0, 2, 3, 4))
        shadow_half = braket(shadow, half_step)
        shadow_second = braket(shadow, second)
        summed = lax.psum(
            (
                cross_local[0],
                cross_local[1],
                norm_local,
                shadow_half[0],
                shadow_half[1],
                shadow_second[0],
                shadow_second[1],
            ),
            ("gx", "gyz"),
        )
        cross_real, cross_imag, norm_second = (summed[0], summed[1], summed[2])
        omega_step = (cross_real / norm_second, cross_imag / norm_second)
        evolved = evolved + scale_complex(alpha_step, dir_hat) + scale_complex(omega_step, half_hat)
        residual = half_step - scale_complex(omega_step, second)
        if iteration + 1 < ITERS:
            along_second = times_complex(omega_step, (summed[5], summed[6]))
            rho_next = (summed[3] - along_second[0], summed[4] - along_second[1])
            beta_step = times_complex(
                divide_complex(rho_next, rho_now), divide_complex(alpha_step, omega_step)
            )
            direction = residual + scale_complex(
                beta_step, direction - scale_complex(omega_step, image)
            )
            rho_now = rho_next
    return (evolved, residual)


class Layout:
    def __init__(self, groups, rows, columns, count):
        self.groups, self.rows, self.columns, self.count = groups, rows, columns, count
        self.width = -(-count // rows)
        self.segments = columns // self.width
        self.fits = columns % self.width == 0
        inner = [(da, dc) for da in range(rows) for dc in range(self.width)]
        self.near = [(da, 0, dc) for da, dc in inner]
        self.far = [(da, ds, dc) for ds in range(1, self.segments) for da, dc in inner]
        self.across = [(0, ds, 0) for ds in range(1, self.segments)]

    def here(self):
        b = lax.axis_index("gyz")
        return lax.axis_index("gx"), b // self.width, lax.rem(b, self.width)

    def moved(self, place, offset, sign=1):
        sizes = (self.rows, self.segments, self.width)
        return tuple(
            p if o == 0 else lax.rem(p + (o if sign > 0 else n - o), n)
            for p, o, n in zip(place, offset, sizes)
        )

    def solves(self, place):
        return place[0] * self.width + place[2]

    def pairs(self, offset, towards, to_owner):
        found = []
        for g in range(self.groups):
            for a in range(self.rows):
                for b in range(self.columns):
                    place = (a, b // self.width, b % self.width)
                    sizes = (self.rows, self.segments, self.width)
                    other = tuple((p + o) % n for p, o, n in zip(place, offset, sizes))
                    source, target = (place, other) if towards else (other, place)
                    owner = target if to_owner else source
                    if to_owner is None or self.solves(owner) < self.count:
                        found.append((self.linear(g, source), self.linear(g, target)))
        return found

    def linear(self, g, place):
        return (g * self.rows + place[0]) * self.columns + place[1] * self.width + place[2]


def complex_mul(first, second):
    return (
        first[0] * second[0] - first[1] * second[1],
        first[0] * second[1] + first[1] * second[0],
    )


def pack_far_kernel(layout, orbitals_ref, *out_refs):
    here = layout.here()
    for offset, out_ref in zip(layout.far, out_refs):
        q = jnp.minimum(layout.solves(layout.moved(here, offset, -1)), layout.count - 1)
        out_ref[0] = orbitals_ref[0, q]
        out_ref[1] = orbitals_ref[1, q]


def pack_near_kernel(layout, orbitals_ref, potential_ref, *refs):
    others, out_refs = (refs[: len(layout.across)], refs[len(layout.across) :])
    here = layout.here()
    for offset, out_ref in zip(layout.near[1:], out_refs):
        q = jnp.minimum(layout.solves(layout.moved(here, offset, -1)), layout.count - 1)
        out_ref[0] = orbitals_ref[0, q]
        out_ref[1] = orbitals_ref[1, q]
        for slot, ref in enumerate((potential_ref,) + tuple(others)):
            out_ref[2 + slot] = ref[...]


def total(parts):
    return jnp.sum(parts, axis=(0, 1), keepdims=True)


def fold(product):
    return jnp.sum(product.reshape(-1, 8, product.shape[-1]), axis=0)


def solve_kernel(layout, *refs):
    near, far, across = (layout.near, layout.far, layout.across)
    orbitals_ref, potential_ref = refs[:2]
    refs = refs[2:]
    pots, refs = (refs[: len(across)], refs[len(across) :])
    near_refs, refs = (refs[: len(near) - 1], refs[len(near) - 1 :])
    far_refs, refs = (refs[: len(far)], refs[len(far) :])
    outs, scratch = (refs[: len(near)], refs[len(near) :])
    diag, inv, padded_d, padded_h, evolved, res, shadow, direc, image, second = scratch
    bx, by, nz = potential_ref.shape
    nx, ny = (bx * layout.rows, by * layout.columns)
    here = layout.here()

    def corner(offset):
        a, s, c = layout.moved(here, offset)
        return a * bx, pl.multiple_of((s * layout.width + c) * by, 8)

    zero_edge = jnp.zeros((2, 2, ny + 2 * MARGIN, nz), jnp.float32)
    for padded in (padded_d, padded_h):
        padded[:, 0:2] = zero_edge
        padded[:, nx + 2 : nx + 4] = zero_edge
        padded[:, :, 0:MARGIN] = jnp.zeros((2, nx + 4, MARGIN, nz), jnp.float32)
        padded[:, :, ny + MARGIN : ny + 2 * MARGIN] = jnp.zeros((2, nx + 4, MARGIN, nz), jnp.float32)

    def place_orbital(offset, part, block):
        x0, y0 = corner(offset)
        padded_d[part, pl.ds(x0 + 2, bx), pl.ds(y0 + MARGIN, by), :] = block
        evolved[part, pl.ds(x0, bx), pl.ds(y0, by), :] = block

    def place_potential(offset, block):
        x0, y0 = corner(offset)
        d = HALF_STEP * (DIAGONAL + block)
        diag[pl.ds(x0, bx), pl.ds(y0, by), :] = d
        inv[pl.ds(x0, bx), pl.ds(y0, by), :] = K2 / (1.0 + d * d)

    mine = jnp.minimum(layout.solves(here), layout.count - 1)
    place_potential(near[0], potential_ref[...])
    for offset, ref in zip(across, pots):
        place_potential(offset, ref[...])
    for part in range(2):
        place_orbital(near[0], part, orbitals_ref[part, mine])
    for (da, _, dc), ref in zip(near[1:], near_refs):
        for ds in range(layout.segments):
            place_potential((da, ds, dc), ref[2 + ds])
        for part in range(2):
            place_orbital((da, 0, dc), part, ref[part])
    for offset, ref in zip(far, far_refs):
        for part in range(2):
            place_orbital(offset, part, ref[part])

    lane = lax.broadcasted_iota(jnp.int32, (ny, nz), 1)
    keep = {s: (lane >= s if s > 0 else lane < nz + s) for s in (1, -1, 2, -2)}

    def shifted(center, s):
        return jnp.where(keep[s], pltpu.roll(center, s % nz, 1), 0.0)

    def stencil(padded, part, x):
        center = padded[part, x + 2, MARGIN : MARGIN + ny, :]

        def ring(s):
            return (
                (padded[part, x + 2 + s, MARGIN : MARGIN + ny, :] + padded[part, x + 2 - s, MARGIN : MARGIN + ny, :])
                + (padded[part, x + 2, MARGIN + s : MARGIN + s + ny, :] + padded[part, x + 2, MARGIN - s : MARGIN - s + ny, :])
                + (shifted(center, s) + shifted(center, -s))
            )

        return center, ring(2) - RATIO * ring(1)

    def sums(count):
        return tuple(jnp.zeros((8, nz), jnp.float32) for _ in range(count))

    def precondition_at(re, im, x):
        d, scale = (diag[x], inv[x])
        return (re + d * im) * scale, (im - d * re) * scale

    def start(x, acc):
        d = diag[x]
        center_re, off_re = stencil(padded_d, 0, x)
        center_im, off_im = stencil(padded_d, 1, x)
        re = 2.0 * (d * center_im + K2 * off_im)
        im = -2.0 * (d * center_re + K2 * off_re)
        shadow[0, x] = re
        shadow[1, x] = im
        hat_re, hat_im = precondition_at(re, im, x)
        padded_h[0, x + 2, MARGIN : MARGIN + ny, :] = hat_re
        padded_h[1, x + 2, MARGIN : MARGIN + ny, :] = hat_im
        return (acc[0] + fold(re * re + im * im),)

    (norm,) = lax.fori_loop(0, nx, start, sums(1), unroll=8)
    rho = (total(norm), jnp.zeros((1, 1), jnp.float32))
    residual, direction = (shadow, shadow)
    hat, other = (padded_h, padded_d)

    for iteration in range(ITERS):

        def image_at(x, acc):
            _, off_re = stencil(hat, 0, x)
            _, off_im = stencil(hat, 1, x)
            re = direction[0, x] - off_im
            im = direction[1, x] + off_re
            image[0, x] = re
            image[1, x] = im
            s_re, s_im = (shadow[0, x], shadow[1, x])
            return (acc[0] + fold(s_re * re + s_im * im), acc[1] + fold(s_re * im - s_im * re))

        acc = lax.fori_loop(0, nx, image_at, sums(2), unroll=8)
        sigma = (total(acc[0]), total(acc[1]))
        alpha = divide_complex(rho, sigma)

        def half_at(x, acc):
            i_re, i_im = (image[0, x], image[1, x])
            re = residual[0, x] - (alpha[0] * i_re - alpha[1] * i_im)
            im = residual[1, x] - (alpha[0] * i_im + alpha[1] * i_re)
            res[0, x] = re
            res[1, x] = im
            hat_re, hat_im = precondition_at(re, im, x)
            other[0, x + 2, MARGIN : MARGIN + ny, :] = hat_re
            other[1, x + 2, MARGIN : MARGIN + ny, :] = hat_im
            s_re, s_im = (shadow[0, x], shadow[1, x])
            return (acc[0] + fold(s_re * re + s_im * im), acc[1] + fold(s_re * im - s_im * re))

        acc = lax.fori_loop(0, nx, half_at, sums(2), unroll=4)
        shadow_half = (total(acc[0]), total(acc[1]))

        def second_at(x, acc):
            _, off_re = stencil(other, 0, x)
            _, off_im = stencil(other, 1, x)
            h_re, h_im = (res[0, x], res[1, x])
            re = h_re - off_im
            im = h_im + off_re
            second[0, x] = re
            second[1, x] = im
            s_re, s_im = (shadow[0, x], shadow[1, x])
            return (
                acc[0] + fold(re * h_re + im * h_im),
                acc[1] + fold(re * h_im - im * h_re),
                acc[2] + fold(re * re + im * im),
                acc[3] + fold(s_re * re + s_im * im),
                acc[4] + fold(s_re * im - s_im * re),
            )

        acc = lax.fori_loop(0, nx, second_at, sums(5), unroll=8)
        cross_re, cross_im, norm, ss_re, ss_im = [total(part) for part in acc]
        omega = (cross_re / norm, cross_im / norm)
        alpha_hat = (alpha[0] * (1.0 / K2), alpha[1] * (1.0 / K2))
        omega_hat = (omega[0] * (1.0 / K2), omega[1] * (1.0 / K2))

        def step_evolved(base, at_d, at_h):
            along_d = complex_mul(alpha_hat, at_d)
            along_h = complex_mul(omega_hat, at_h)
            return (base[0] + (along_d[0] + along_h[0]), base[1] + (along_d[1] + along_h[1]))

        if iteration + 1 < ITERS:
            moved = complex_mul(omega, (ss_re, ss_im))
            rho_next = (shadow_half[0] - moved[0], shadow_half[1] - moved[1])
            beta = complex_mul(divide_complex(rho_next, rho), divide_complex(alpha, omega))
            beta_omega = complex_mul(beta, omega)
            rho = rho_next

            def update_at(x, carry):
                at_d = (hat[0, x + 2, MARGIN : MARGIN + ny, :], hat[1, x + 2, MARGIN : MARGIN + ny, :])
                at_h = (other[0, x + 2, MARGIN : MARGIN + ny, :], other[1, x + 2, MARGIN : MARGIN + ny, :])
                e = step_evolved((evolved[0, x], evolved[1, x]), at_d, at_h)
                evolved[0, x] = e[0]
                evolved[1, x] = e[1]
                w = complex_mul(omega, (second[0, x], second[1, x]))
                r_re = res[0, x] - w[0]
                r_im = res[1, x] - w[1]
                res[0, x] = r_re
                res[1, x] = r_im
                p = complex_mul(beta, (direction[0, x], direction[1, x]))
                v = complex_mul(beta_omega, (image[0, x], image[1, x]))
                p_re = r_re + (p[0] - v[0])
                p_im = r_im + (p[1] - v[1])
                direc[0, x] = p_re
                direc[1, x] = p_im
                hat_re, hat_im = precondition_at(p_re, p_im, x)
                hat[0, x + 2, MARGIN : MARGIN + ny, :] = hat_re
                hat[1, x + 2, MARGIN : MARGIN + ny, :] = hat_im
                return carry

            lax.fori_loop(0, nx, update_at, 0, unroll=4)
            residual, direction = (res, direc)
        else:
            for offset, out in zip(near, outs):
                x0, y0 = corner(offset)

                def finish_at(i, carry):
                    x, y = (x0 + i, pl.ds(y0, by))
                    yp = pl.ds(y0 + MARGIN, by)
                    at_d = (hat[0, x + 2, yp, :], hat[1, x + 2, yp, :])
                    at_h = (other[0, x + 2, yp, :], other[1, x + 2, yp, :])
                    e = step_evolved((evolved[0, x, y, :], evolved[1, x, y, :]), at_d, at_h)
                    w = complex_mul(omega, (second[0, x, y, :], second[1, x, y, :]))
                    out[0, i] = e[0]
                    out[1, i] = e[1]
                    out[2, i] = res[0, x, y, :] - w[0]
                    out[3, i] = res[1, x, y, :] - w[1]
                    return carry

                lax.fori_loop(0, bx, finish_at, 0)


def unpack_kernel(layout, *refs):
    blocks, (evolved_ref, residual_ref) = (refs[: len(layout.near)], refs[len(layout.near) :])
    here = layout.here()
    for offset, block in zip(layout.near, blocks):
        q = layout.solves(layout.moved(here, offset, -1))

        @pl.when(q < layout.count)
        def _():
            for part in range(2):
                evolved_ref[part, q] = block[part]
                residual_ref[part, q] = block[2 + part]


VMEM_SPEC = pl.BlockSpec(memory_space=pltpu.VMEM)


def whole_call(kernel, name, operands, out_shapes, limit, scratch=()):
    return pl.pallas_call(
        kernel,
        out_shape=[jax.ShapeDtypeStruct(dims, jnp.float32) for dims in out_shapes],
        in_specs=[VMEM_SPEC] * len(operands),
        out_specs=[VMEM_SPEC] * len(out_shapes),
        scratch_shapes=list(scratch),
        compiler_params=pltpu.CompilerParams(vmem_limit_bytes=limit),
        name=name,
    )(*operands)


def solve_scratch(nx, ny, nz):
    field = pltpu.VMEM((2, nx, ny, nz), jnp.float32)
    padded = pltpu.VMEM((2, nx + 4, ny + 2 * MARGIN, nz), jnp.float32)
    scalar_field = pltpu.VMEM((nx, ny, nz), jnp.float32)
    return [scalar_field] * 2 + [padded] * 2 + [field] * 6


def gathered(layout, orbitals, potential):
    _, _, bx, by, nz = orbitals.shape
    axes = ("orb", "gx", "gyz")
    near, far, across = (layout.near, layout.far, layout.across)
    slots = 2 + layout.segments

    def fetch(array, offset, to_owner):
        return lax.ppermute(array, axes, layout.pairs(offset, False, to_owner))

    pots = [fetch(potential, offset, None) for offset in across]
    far_messages = whole_call(
        functools.partial(pack_far_kernel, layout),
        "pack_far",
        [orbitals],
        [(2, bx, by, nz)] * len(far),
        4 * 2**20,
    )
    far_blocks = [fetch(m, offset, True) for offset, m in zip(far, far_messages)]
    near_messages = whole_call(
        functools.partial(pack_near_kernel, layout),
        "pack_near",
        [orbitals, potential] + pots,
        [(slots, bx, by, nz)] * (len(near) - 1),
        4 * 2**20,
    )
    near_blocks = [fetch(m, offset, True) for offset, m in zip(near[1:], near_messages)]
    pieces = whole_call(
        functools.partial(solve_kernel, layout),
        "solve",
        [orbitals, potential] + pots + near_blocks + far_blocks,
        [(4, bx, by, nz)] * len(near),
        28 * 2**20,
        solve_scratch(bx * layout.rows, by * layout.columns, nz),
    )
    arrived = [pieces[0]]
    for offset, piece in zip(near[1:], pieces[1:]):
        arrived.append(lax.ppermute(piece, axes, layout.pairs(offset, True, False)))
    return whole_call(
        functools.partial(unpack_kernel, layout),
        "unpack",
        arrived,
        [orbitals.shape] * 2,
        6 * 2**20,
    )


def solution(mesh):
    sizes = dict(mesh.shape)

    def shards(orbitals, potential):
        _, count, bx, by, nz = orbitals.shape
        layout = Layout(sizes["orb"], sizes["gx"], sizes["gyz"], count)
        nx, ny = (bx * layout.rows, by * layout.columns)
        fields = 24 * 4 * (nx + 4) * (ny + 2 * MARGIN) * nz
        if layout.fits and fields <= WORKING_SET and by % 8 == 0 and nz % 128 == 0:
            return tuple(gathered(layout, orbitals, potential))
        return distributed(orbitals, potential)

    return jax.shard_map(
        shards,
        mesh=mesh,
        in_specs=(P(None, "orb", "gx", "gyz", None), P("gx", "gyz", None)),
        out_specs=(P(None, "orb", "gx", "gyz", None), P(None, "orb", "gx", "gyz", None)),
        check_vma=False,
    )
```

```python
import functools

import jax
import jax.numpy as jnp
from jax import lax
from jax.experimental import pallas as pl
from jax.experimental.pallas import tpu as pltpu
from jax.sharding import PartitionSpec as P


ITERS = 4


SPACING = 0.25
HALF_STEP = 0.05
COEFF_NEAR = 4.0 / 3.0
COEFF_FAR = -1.0 / 12.0
COEFF_SELF = -2.5

RATIO = -COEFF_NEAR / COEFF_FAR
K2 = HALF_STEP * -0.5 / SPACING**2 * COEFF_FAR
DIAGONAL = -0.5 / SPACING**2 * 3.0 * COEFF_SELF
MARGIN = 8
WORKING_SET = 40 * 2**20


def with_halo(array, sides, width):
    for axis, dim in sides:
        size, length = (lax.axis_size(axis), array.shape[dim])
        up = [(i, (i + 1) % size) for i in range(size - 1)]
        down = [(j, i) for i, j in up]
        last = lax.slice_in_dim(array, length - width, length, axis=dim)
        leading = lax.slice_in_dim(array, 0, width, axis=dim)
        before = lax.ppermute(last, axis, up)
        after = lax.ppermute(leading, axis, down)
        array = jnp.concatenate([before, array, after], axis=dim)
    return array


def laplace_apply(padded, potential):
    extent = (padded.shape[2] - 4, padded.shape[3] - 4, padded.shape[4] - 4)

    def window(shift_x, shift_y, shift_z):
        return padded[
            :,
            :,
            2 + shift_x : 2 + shift_x + extent[0],
            2 + shift_y : 2 + shift_y + extent[1],
            2 + shift_z : 2 + shift_z + extent[2],
        ]

    center = window(0, 0, 0)
    summed = 3.0 * COEFF_SELF * center
    for offset, weight in ((1, COEFF_NEAR), (2, COEFF_FAR)):
        summed = summed + weight * (
            window(offset, 0, 0)
            + window(-offset, 0, 0)
            + window(0, offset, 0)
            + window(0, -offset, 0)
            + window(0, 0, offset)
            + window(0, 0, -offset)
        )
    return -0.5 / SPACING**2 * summed + potential * center


def pad_depth(vector):
    return jnp.pad(vector, ((0, 0), (0, 0), (0, 0), (0, 0), (2, 2)))


def system(vector, applied):
    return jnp.stack([vector[0] - HALF_STEP * applied[1], vector[1] + HALF_STEP * applied[0]])


def precondition(vector, potential):
    diagonal = HALF_STEP * (3.75 / SPACING**2 + potential)
    divisor = 1.0 + diagonal * diagonal
    return jnp.stack(
        [(vector[0] + diagonal * vector[1]) / divisor, (vector[1] - diagonal * vector[0]) / divisor]
    )


def braket(left, right):
    real_part = jnp.sum(left[0] * right[0] + left[1] * right[1], axis=(1, 2, 3))
    imag_part = jnp.sum(left[0] * right[1] - left[1] * right[0], axis=(1, 2, 3))
    return (real_part, imag_part)


def times_complex(first, second):
    return (
        first[0] * second[0] - first[1] * second[1],
        first[0] * second[1] + first[1] * second[0],
    )


def divide_complex(first, second):
    modulus = second[0] * second[0] + second[1] * second[1]
    return (
        (first[0] * second[0] + first[1] * second[1]) / modulus,
        (first[1] * second[0] - first[0] * second[1]) / modulus,
    )


def scale_complex(coeff, vector):
    real_coef = coeff[0][:, None, None, None]
    imag_coef = coeff[1][:, None, None, None]
    return jnp.stack(
        [
            real_coef * vector[0] - imag_coef * vector[1],
            real_coef * vector[1] + imag_coef * vector[0],
        ]
    )


def distributed(orbitals, potential):
    def apply_shallow(vector):
        padded = with_halo(vector, (("gx", 2), ("gyz", 3)), 2)
        return laplace_apply(pad_depth(padded), potential)

    h_orbitals = apply_shallow(orbitals)
    residual = jnp.stack([2.0 * HALF_STEP * h_orbitals[1], -2.0 * HALF_STEP * h_orbitals[0]])
    evolved = orbitals
    shadow = residual
    direction = residual
    rho_now = lax.psum(braket(shadow, residual), ("gx", "gyz"))
    for iteration in range(ITERS):
        dir_hat = precondition(direction, potential)
        image = system(dir_hat, apply_shallow(dir_hat))
        alpha_step = divide_complex(rho_now, lax.psum(braket(shadow, image), ("gx", "gyz")))
        half_step = residual - scale_complex(alpha_step, image)
        half_hat = precondition(half_step, potential)
        second = system(half_hat, apply_shallow(half_hat))
        cross_local = braket(second, half_step)
        norm_local = jnp.sum(second * second, axis=(0, 2, 3, 4))
        shadow_half = braket(shadow, half_step)
        shadow_second = braket(shadow, second)
        summed = lax.psum(
            (
                cross_local[0],
                cross_local[1],
                norm_local,
                shadow_half[0],
                shadow_half[1],
                shadow_second[0],
                shadow_second[1],
            ),
            ("gx", "gyz"),
        )
        cross_real, cross_imag, norm_second = (summed[0], summed[1], summed[2])
        omega_step = (cross_real / norm_second, cross_imag / norm_second)
        evolved = evolved + scale_complex(alpha_step, dir_hat) + scale_complex(omega_step, half_hat)
        residual = half_step - scale_complex(omega_step, second)
        if iteration + 1 < ITERS:
            along_second = times_complex(omega_step, (summed[5], summed[6]))
            rho_next = (summed[3] - along_second[0], summed[4] - along_second[1])
            beta_step = times_complex(
                divide_complex(rho_next, rho_now), divide_complex(alpha_step, omega_step)
            )
            direction = residual + scale_complex(
                beta_step, direction - scale_complex(omega_step, image)
            )
            rho_now = rho_next
    return (evolved, residual)


class Layout:
    def __init__(self, groups, rows, columns, count):
        self.groups, self.rows, self.columns, self.count = groups, rows, columns, count
        self.width = -(-count // rows)
        self.segments = columns // self.width
        self.fits = columns % self.width == 0
        inner = [(da, dc) for da in range(rows) for dc in range(self.width)]
        self.near = [(da, 0, dc) for da, dc in inner]
        self.far = [(da, ds, dc) for ds in range(1, self.segments) for da, dc in inner]
        self.across = [(0, ds, 0) for ds in range(1, self.segments)]

    def here(self):
        b = lax.axis_index("gyz")
        return lax.axis_index("gx"), b // self.width, lax.rem(b, self.width)

    def moved(self, place, offset, sign=1):
        sizes = (self.rows, self.segments, self.width)
        return tuple(
            p if o == 0 else lax.rem(p + (o if sign > 0 else n - o), n)
            for p, o, n in zip(place, offset, sizes)
        )

    def solves(self, place):
        return place[0] * self.width + place[2]

    def pairs(self, offset, towards, to_owner):
        found = []
        for g in range(self.groups):
            for a in range(self.rows):
                for b in range(self.columns):
                    place = (a, b // self.width, b % self.width)
                    sizes = (self.rows, self.segments, self.width)
                    other = tuple((p + o) % n for p, o, n in zip(place, offset, sizes))
                    source, target = (place, other) if towards else (other, place)
                    owner = target if to_owner else source
                    if to_owner is None or self.solves(owner) < self.count:
                        found.append((self.linear(g, source), self.linear(g, target)))
        return found

    def linear(self, g, place):
        return (g * self.rows + place[0]) * self.columns + place[1] * self.width + place[2]


def complex_mul(first, second):
    return (
        first[0] * second[0] - first[1] * second[1],
        first[0] * second[1] + first[1] * second[0],
    )


def pack_far_kernel(layout, orbitals_ref, potential_ref, *out_refs):
    here = layout.here()
    for offset, out_ref in zip(layout.far, out_refs):
        q = jnp.minimum(layout.solves(layout.moved(here, offset, -1)), layout.count - 1)
        out_ref[0] = orbitals_ref[0, q]
        out_ref[1] = orbitals_ref[1, q]
        if offset in layout.across:
            out_ref[2] = potential_ref[...]


def pack_near_kernel(layout, orbitals_ref, potential_ref, *refs):
    others, out_refs = (refs[: len(layout.across)], refs[len(layout.across) :])
    here = layout.here()
    for offset, out_ref in zip(layout.near[1:], out_refs):
        q = jnp.minimum(layout.solves(layout.moved(here, offset, -1)), layout.count - 1)
        out_ref[0] = orbitals_ref[0, q]
        out_ref[1] = orbitals_ref[1, q]
        for slot, ref in enumerate((potential_ref,) + tuple(others)):
            out_ref[2 + slot] = ref[...] if slot == 0 else ref[2]


def total(parts):
    return jnp.sum(parts, axis=(0, 1), keepdims=True)


def fold(product):
    return jnp.sum(product.reshape(-1, 8, product.shape[-1]), axis=0)


def solve_kernel(layout, *refs):
    near, far, across = (layout.near, layout.far, layout.across)
    orbitals_ref, potential_ref = refs[:2]
    refs = refs[2:]
    near_refs, refs = (refs[: len(near) - 1], refs[len(near) - 1 :])
    far_refs, refs = (refs[: len(far)], refs[len(far) :])
    outs, scratch = (refs[: len(near)], refs[len(near) :])
    diag, inv, padded_d, padded_h, evolved, res, shadow, direc, image, second = scratch
    bx, by, nz = potential_ref.shape
    nx, ny = (bx * layout.rows, by * layout.columns)
    here = layout.here()

    def corner(offset):
        a, s, c = layout.moved(here, offset)
        return a * bx, pl.multiple_of((s * layout.width + c) * by, 8)

    zero_edge = jnp.zeros((2, 2, ny + 2 * MARGIN, nz), jnp.float32)
    for padded in (padded_d, padded_h):
        padded[:, 0:2] = zero_edge
        padded[:, nx + 2 : nx + 4] = zero_edge
        padded[:, :, 0:MARGIN] = jnp.zeros((2, nx + 4, MARGIN, nz), jnp.float32)
        padded[:, :, ny + MARGIN : ny + 2 * MARGIN] = jnp.zeros((2, nx + 4, MARGIN, nz), jnp.float32)

    def place_orbital(offset, part, block):
        x0, y0 = corner(offset)
        padded_d[part, pl.ds(x0 + 2, bx), pl.ds(y0 + MARGIN, by), :] = block
        evolved[part, pl.ds(x0, bx), pl.ds(y0, by), :] = block

    def place_potential(offset, block):
        x0, y0 = corner(offset)
        d = HALF_STEP * (DIAGONAL + block)
        diag[pl.ds(x0, bx), pl.ds(y0, by), :] = d
        inv[pl.ds(x0, bx), pl.ds(y0, by), :] = K2 / (1.0 + d * d)

    mine = jnp.minimum(layout.solves(here), layout.count - 1)
    place_potential(near[0], potential_ref[...])
    for part in range(2):
        place_orbital(near[0], part, orbitals_ref[part, mine])
    for (da, _, dc), ref in zip(near[1:], near_refs):
        for ds in range(layout.segments):
            place_potential((da, ds, dc), ref[2 + ds])
        for part in range(2):
            place_orbital((da, 0, dc), part, ref[part])
    for offset, ref in zip(far, far_refs):
        if offset in across:
            place_potential(offset, ref[2])
        for part in range(2):
            place_orbital(offset, part, ref[part])

    lane = lax.broadcasted_iota(jnp.int32, (ny, nz), 1)
    keep = {s: (lane >= s if s > 0 else lane < nz + s) for s in (1, -1, 2, -2)}

    def shifted(center, s):
        return jnp.where(keep[s], pltpu.roll(center, s % nz, 1), 0.0)

    def stencil(padded, part, x):
        center = padded[part, x + 2, MARGIN : MARGIN + ny, :]

        def ring(s):
            return (
                (padded[part, x + 2 + s, MARGIN : MARGIN + ny, :] + padded[part, x + 2 - s, MARGIN : MARGIN + ny, :])
                + (padded[part, x + 2, MARGIN + s : MARGIN + s + ny, :] + padded[part, x + 2, MARGIN - s : MARGIN - s + ny, :])
                + (shifted(center, s) + shifted(center, -s))
            )

        return center, ring(2) - RATIO * ring(1)

    def sums(count):
        return tuple(jnp.zeros((8, nz), jnp.float32) for _ in range(count))

    def precondition_at(re, im, x):
        d, scale = (diag[x], inv[x])
        return (re + d * im) * scale, (im - d * re) * scale

    def start(x, acc):
        d = diag[x]
        center_re, off_re = stencil(padded_d, 0, x)
        center_im, off_im = stencil(padded_d, 1, x)
        re = 2.0 * (d * center_im + K2 * off_im)
        im = -2.0 * (d * center_re + K2 * off_re)
        shadow[0, x] = re
        shadow[1, x] = im
        hat_re, hat_im = precondition_at(re, im, x)
        padded_h[0, x + 2, MARGIN : MARGIN + ny, :] = hat_re
        padded_h[1, x + 2, MARGIN : MARGIN + ny, :] = hat_im
        return (acc[0] + fold(re * re + im * im),)

    (norm,) = lax.fori_loop(0, nx, start, sums(1), unroll=8)
    rho = (total(norm), jnp.zeros((1, 1), jnp.float32))
    residual, direction = (shadow, shadow)
    hat, other = (padded_h, padded_d)

    for iteration in range(ITERS):

        def image_at(x, acc):
            _, off_re = stencil(hat, 0, x)
            _, off_im = stencil(hat, 1, x)
            re = direction[0, x] - off_im
            im = direction[1, x] + off_re
            image[0, x] = re
            image[1, x] = im
            s_re, s_im = (shadow[0, x], shadow[1, x])
            return (acc[0] + fold(s_re * re + s_im * im), acc[1] + fold(s_re * im - s_im * re))

        acc = lax.fori_loop(0, nx, image_at, sums(2), unroll=8)
        sigma = (total(acc[0]), total(acc[1]))
        alpha = divide_complex(rho, sigma)

        def half_at(x, acc):
            i_re, i_im = (image[0, x], image[1, x])
            re = residual[0, x] - (alpha[0] * i_re - alpha[1] * i_im)
            im = residual[1, x] - (alpha[0] * i_im + alpha[1] * i_re)
            res[0, x] = re
            res[1, x] = im
            hat_re, hat_im = precondition_at(re, im, x)
            other[0, x + 2, MARGIN : MARGIN + ny, :] = hat_re
            other[1, x + 2, MARGIN : MARGIN + ny, :] = hat_im
            s_re, s_im = (shadow[0, x], shadow[1, x])
            return (acc[0] + fold(s_re * re + s_im * im), acc[1] + fold(s_re * im - s_im * re))

        acc = lax.fori_loop(0, nx, half_at, sums(2), unroll=4)
        shadow_half = (total(acc[0]), total(acc[1]))

        def second_at(x, acc):
            _, off_re = stencil(other, 0, x)
            _, off_im = stencil(other, 1, x)
            h_re, h_im = (res[0, x], res[1, x])
            re = h_re - off_im
            im = h_im + off_re
            second[0, x] = re
            second[1, x] = im
            s_re, s_im = (shadow[0, x], shadow[1, x])
            return (
                acc[0] + fold(re * h_re + im * h_im),
                acc[1] + fold(re * h_im - im * h_re),
                acc[2] + fold(re * re + im * im),
                acc[3] + fold(s_re * re + s_im * im),
                acc[4] + fold(s_re * im - s_im * re),
            )

        acc = lax.fori_loop(0, nx, second_at, sums(5), unroll=8)
        cross_re, cross_im, norm, ss_re, ss_im = [total(part) for part in acc]
        omega = (cross_re / norm, cross_im / norm)
        alpha_hat = (alpha[0] * (1.0 / K2), alpha[1] * (1.0 / K2))
        omega_hat = (omega[0] * (1.0 / K2), omega[1] * (1.0 / K2))

        def step_evolved(base, at_d, at_h):
            along_d = complex_mul(alpha_hat, at_d)
            along_h = complex_mul(omega_hat, at_h)
            return (base[0] + (along_d[0] + along_h[0]), base[1] + (along_d[1] + along_h[1]))

        if iteration + 1 < ITERS:
            moved = complex_mul(omega, (ss_re, ss_im))
            rho_next = (shadow_half[0] - moved[0], shadow_half[1] - moved[1])
            beta = complex_mul(divide_complex(rho_next, rho), divide_complex(alpha, omega))
            beta_omega = complex_mul(beta, omega)
            rho = rho_next

            def update_at(x, carry):
                at_d = (hat[0, x + 2, MARGIN : MARGIN + ny, :], hat[1, x + 2, MARGIN : MARGIN + ny, :])
                at_h = (other[0, x + 2, MARGIN : MARGIN + ny, :], other[1, x + 2, MARGIN : MARGIN + ny, :])
                e = step_evolved((evolved[0, x], evolved[1, x]), at_d, at_h)
                evolved[0, x] = e[0]
                evolved[1, x] = e[1]
                w = complex_mul(omega, (second[0, x], second[1, x]))
                r_re = res[0, x] - w[0]
                r_im = res[1, x] - w[1]
                res[0, x] = r_re
                res[1, x] = r_im
                p = complex_mul(beta, (direction[0, x], direction[1, x]))
                v = complex_mul(beta_omega, (image[0, x], image[1, x]))
                p_re = r_re + (p[0] - v[0])
                p_im = r_im + (p[1] - v[1])
                direc[0, x] = p_re
                direc[1, x] = p_im
                hat_re, hat_im = precondition_at(p_re, p_im, x)
                hat[0, x + 2, MARGIN : MARGIN + ny, :] = hat_re
                hat[1, x + 2, MARGIN : MARGIN + ny, :] = hat_im
                return carry

            lax.fori_loop(0, nx, update_at, 0, unroll=4)
            residual, direction = (res, direc)
        else:
            for offset, out in zip(near, outs):
                x0, y0 = corner(offset)

                def finish_at(i, carry):
                    x, y = (x0 + i, pl.ds(y0, by))
                    yp = pl.ds(y0 + MARGIN, by)
                    at_d = (hat[0, x + 2, yp, :], hat[1, x + 2, yp, :])
                    at_h = (other[0, x + 2, yp, :], other[1, x + 2, yp, :])
                    e = step_evolved((evolved[0, x, y, :], evolved[1, x, y, :]), at_d, at_h)
                    w = complex_mul(omega, (second[0, x, y, :], second[1, x, y, :]))
                    out[0, i] = e[0]
                    out[1, i] = e[1]
                    out[2, i] = res[0, x, y, :] - w[0]
                    out[3, i] = res[1, x, y, :] - w[1]
                    return carry

                lax.fori_loop(0, bx, finish_at, 0)


def unpack_kernel(layout, *refs):
    blocks, (evolved_ref, residual_ref) = (refs[: len(layout.near)], refs[len(layout.near) :])
    here = layout.here()
    for offset, block in zip(layout.near, blocks):
        q = layout.solves(layout.moved(here, offset, -1))

        @pl.when(q < layout.count)
        def _():
            for part in range(2):
                evolved_ref[part, q] = block[part]
                residual_ref[part, q] = block[2 + part]


VMEM_SPEC = pl.BlockSpec(memory_space=pltpu.VMEM)


def whole_call(kernel, operands, out_shapes, limit, scratch=()):
    return pl.pallas_call(
        kernel,
        out_shape=[jax.ShapeDtypeStruct(dims, jnp.float32) for dims in out_shapes],
        in_specs=[VMEM_SPEC] * len(operands),
        out_specs=[VMEM_SPEC] * len(out_shapes),
        scratch_shapes=list(scratch),
        compiler_params=pltpu.CompilerParams(vmem_limit_bytes=limit),
    )(*operands)


def solve_scratch(nx, ny, nz):
    field = pltpu.VMEM((2, nx, ny, nz), jnp.float32)
    padded = pltpu.VMEM((2, nx + 4, ny + 2 * MARGIN, nz), jnp.float32)
    scalar_field = pltpu.VMEM((nx, ny, nz), jnp.float32)
    return [scalar_field] * 2 + [padded] * 2 + [field] * 6


def gathered(layout, orbitals, potential):
    _, _, bx, by, nz = orbitals.shape
    axes = ("orb", "gx", "gyz")
    near, far, across = (layout.near, layout.far, layout.across)
    slots = 2 + layout.segments

    def fetch(array, offset, to_owner):
        return lax.ppermute(array, axes, layout.pairs(offset, False, to_owner))

    far_messages = whole_call(
        functools.partial(pack_far_kernel, layout),
        [orbitals, potential],
        [(3 if offset in across else 2, bx, by, nz) for offset in far],
        4 * 2**20,
    )
    far_blocks = []
    for offset, message in zip(far, far_messages):
        far_blocks.append(fetch(message, offset, None if offset in across else True))
    pots = [far_blocks[far.index(offset)] for offset in across]
    near_messages = whole_call(
        functools.partial(pack_near_kernel, layout),
        [orbitals, potential] + pots,
        [(slots, bx, by, nz)] * (len(near) - 1),
        4 * 2**20,
    )
    near_blocks = []
    for offset, message in zip(near[1:], near_messages):
        near_blocks.append(fetch(message, offset, True))
    pieces = whole_call(
        functools.partial(solve_kernel, layout),
        [orbitals, potential] + near_blocks + far_blocks,
        [(4, bx, by, nz)] * len(near),
        28 * 2**20,
        solve_scratch(bx * layout.rows, by * layout.columns, nz),
    )
    arrived = [pieces[0]]
    for offset, piece in zip(near[1:], pieces[1:]):
        arrived.append(lax.ppermute(piece, axes, layout.pairs(offset, True, False)))
    return whole_call(
        functools.partial(unpack_kernel, layout), arrived, [orbitals.shape] * 2, 6 * 2**20
    )


def solution(mesh):
    sizes = dict(mesh.shape)

    def shards(orbitals, potential):
        _, count, bx, by, nz = orbitals.shape
        layout = Layout(sizes["orb"], sizes["gx"], sizes["gyz"], count)
        nx, ny = (bx * layout.rows, by * layout.columns)
        fields = 24 * 4 * (nx + 4) * (ny + 2 * MARGIN) * nz
        if layout.fits and fields <= WORKING_SET and by % 8 == 0 and nz % 128 == 0:
            return tuple(gathered(layout, orbitals, potential))
        return distributed(orbitals, potential)

    return jax.shard_map(
        shards,
        mesh=mesh,
        in_specs=(P(None, "orb", "gx", "gyz", None), P("gx", "gyz", None)),
        out_specs=(P(None, "orb", "gx", "gyz", None), P(None, "orb", "gx", "gyz", None)),
        check_vma=False,
    )
```

```python
import functools

import jax
import jax.numpy as jnp
from jax import lax
from jax.experimental import pallas as pl
from jax.experimental.pallas import tpu as pltpu
from jax.sharding import PartitionSpec as P


ITERS = 4


SPACING = 0.25
HALF_STEP = 0.05
COEFF_NEAR = 4.0 / 3.0
COEFF_FAR = -1.0 / 12.0
COEFF_SELF = -2.5

RATIO = -COEFF_NEAR / COEFF_FAR
K2 = HALF_STEP * -0.5 / SPACING**2 * COEFF_FAR
DIAGONAL = -0.5 / SPACING**2 * 3.0 * COEFF_SELF
MARGIN = 8
WORKING_SET = 40 * 2**20


def with_halo(array, sides, width):
    for axis, dim in sides:
        size, length = (lax.axis_size(axis), array.shape[dim])
        up = [(i, (i + 1) % size) for i in range(size - 1)]
        down = [(j, i) for i, j in up]
        last = lax.slice_in_dim(array, length - width, length, axis=dim)
        leading = lax.slice_in_dim(array, 0, width, axis=dim)
        before = lax.ppermute(last, axis, up)
        after = lax.ppermute(leading, axis, down)
        array = jnp.concatenate([before, array, after], axis=dim)
    return array


def laplace_apply(padded, potential):
    extent = (padded.shape[2] - 4, padded.shape[3] - 4, padded.shape[4] - 4)

    def window(shift_x, shift_y, shift_z):
        return padded[
            :,
            :,
            2 + shift_x : 2 + shift_x + extent[0],
            2 + shift_y : 2 + shift_y + extent[1],
            2 + shift_z : 2 + shift_z + extent[2],
        ]

    center = window(0, 0, 0)
    summed = 3.0 * COEFF_SELF * center
    for offset, weight in ((1, COEFF_NEAR), (2, COEFF_FAR)):
        summed = summed + weight * (
            window(offset, 0, 0)
            + window(-offset, 0, 0)
            + window(0, offset, 0)
            + window(0, -offset, 0)
            + window(0, 0, offset)
            + window(0, 0, -offset)
        )
    return -0.5 / SPACING**2 * summed + potential * center


def pad_depth(vector):
    return jnp.pad(vector, ((0, 0), (0, 0), (0, 0), (0, 0), (2, 2)))


def system(vector, applied):
    return jnp.stack([vector[0] - HALF_STEP * applied[1], vector[1] + HALF_STEP * applied[0]])


def precondition(vector, potential):
    diagonal = HALF_STEP * (3.75 / SPACING**2 + potential)
    divisor = 1.0 + diagonal * diagonal
    return jnp.stack(
        [(vector[0] + diagonal * vector[1]) / divisor, (vector[1] - diagonal * vector[0]) / divisor]
    )


def braket(left, right):
    real_part = jnp.sum(left[0] * right[0] + left[1] * right[1], axis=(1, 2, 3))
    imag_part = jnp.sum(left[0] * right[1] - left[1] * right[0], axis=(1, 2, 3))
    return (real_part, imag_part)


def times_complex(first, second):
    return (
        first[0] * second[0] - first[1] * second[1],
        first[0] * second[1] + first[1] * second[0],
    )


def divide_complex(first, second):
    modulus = second[0] * second[0] + second[1] * second[1]
    return (
        (first[0] * second[0] + first[1] * second[1]) / modulus,
        (first[1] * second[0] - first[0] * second[1]) / modulus,
    )


def scale_complex(coeff, vector):
    real_coef = coeff[0][:, None, None, None]
    imag_coef = coeff[1][:, None, None, None]
    return jnp.stack(
        [
            real_coef * vector[0] - imag_coef * vector[1],
            real_coef * vector[1] + imag_coef * vector[0],
        ]
    )


def distributed(orbitals, potential):
    def apply_shallow(vector):
        padded = with_halo(vector, (("gx", 2), ("gyz", 3)), 2)
        return laplace_apply(pad_depth(padded), potential)

    h_orbitals = apply_shallow(orbitals)
    residual = jnp.stack([2.0 * HALF_STEP * h_orbitals[1], -2.0 * HALF_STEP * h_orbitals[0]])
    evolved = orbitals
    shadow = residual
    direction = residual
    rho_now = lax.psum(braket(shadow, residual), ("gx", "gyz"))
    for iteration in range(ITERS):
        dir_hat = precondition(direction, potential)
        image = system(dir_hat, apply_shallow(dir_hat))
        alpha_step = divide_complex(rho_now, lax.psum(braket(shadow, image), ("gx", "gyz")))
        half_step = residual - scale_complex(alpha_step, image)
        half_hat = precondition(half_step, potential)
        second = system(half_hat, apply_shallow(half_hat))
        cross_local = braket(second, half_step)
        norm_local = jnp.sum(second * second, axis=(0, 2, 3, 4))
        shadow_half = braket(shadow, half_step)
        shadow_second = braket(shadow, second)
        summed = lax.psum(
            (
                cross_local[0],
                cross_local[1],
                norm_local,
                shadow_half[0],
                shadow_half[1],
                shadow_second[0],
                shadow_second[1],
            ),
            ("gx", "gyz"),
        )
        cross_real, cross_imag, norm_second = (summed[0], summed[1], summed[2])
        omega_step = (cross_real / norm_second, cross_imag / norm_second)
        evolved = evolved + scale_complex(alpha_step, dir_hat) + scale_complex(omega_step, half_hat)
        residual = half_step - scale_complex(omega_step, second)
        if iteration + 1 < ITERS:
            along_second = times_complex(omega_step, (summed[5], summed[6]))
            rho_next = (summed[3] - along_second[0], summed[4] - along_second[1])
            beta_step = times_complex(
                divide_complex(rho_next, rho_now), divide_complex(alpha_step, omega_step)
            )
            direction = residual + scale_complex(
                beta_step, direction - scale_complex(omega_step, image)
            )
            rho_now = rho_next
    return (evolved, residual)


class Layout:
    def __init__(self, groups, rows, columns, count):
        self.groups, self.rows, self.columns, self.count = groups, rows, columns, count
        self.width = -(-count // rows)
        self.segments = columns // self.width
        self.fits = columns % self.width == 0
        inner = [(da, dc) for da in range(rows) for dc in range(self.width)]
        self.near = [(da, 0, dc) for da, dc in inner]
        self.far = [(da, ds, dc) for ds in range(1, self.segments) for da, dc in inner]
        self.across = [(0, ds, 0) for ds in range(1, self.segments)]

    def here(self):
        b = lax.axis_index("gyz")
        return lax.axis_index("gx"), b // self.width, lax.rem(b, self.width)

    def solved_by(self, place):
        q = self.solves(place)
        return jnp.where(lax.rem(lax.axis_index("orb"), 2) == 0, q, self.rows * self.width - 1 - q)

    def moved(self, place, offset, sign=1):
        sizes = (self.rows, self.segments, self.width)
        return tuple(
            p if o == 0 else lax.rem(p + (o if sign > 0 else n - o), n)
            for p, o, n in zip(place, offset, sizes)
        )

    def solves(self, place):
        return place[0] * self.width + place[2]

    def pairs(self, offset, towards, to_owner):
        found = []
        for g in range(self.groups):
            for a in range(self.rows):
                for b in range(self.columns):
                    place = (a, b // self.width, b % self.width)
                    sizes = (self.rows, self.segments, self.width)
                    other = tuple((p + o) % n for p, o, n in zip(place, offset, sizes))
                    source, target = (place, other) if towards else (other, place)
                    q = self.solves(target if to_owner else source)
                    q = q if g % 2 == 0 else self.rows * self.width - 1 - q
                    if to_owner is None or q < self.count:
                        found.append((self.linear(g, source), self.linear(g, target)))
        return found

    def linear(self, g, place):
        return (g * self.rows + place[0]) * self.columns + place[1] * self.width + place[2]


def complex_mul(first, second):
    return (
        first[0] * second[0] - first[1] * second[1],
        first[0] * second[1] + first[1] * second[0],
    )


def pack_far_kernel(layout, orbitals_ref, *out_refs):
    here = layout.here()
    for offset, out_ref in zip(layout.far, out_refs):
        q = jnp.minimum(layout.solved_by(layout.moved(here, offset, -1)), layout.count - 1)
        out_ref[0] = orbitals_ref[0, q]
        out_ref[1] = orbitals_ref[1, q]


def pack_near_kernel(layout, orbitals_ref, potential_ref, *refs):
    others, out_refs = (refs[: len(layout.across)], refs[len(layout.across) :])
    here = layout.here()
    for offset, out_ref in zip(layout.near[1:], out_refs):
        q = jnp.minimum(layout.solved_by(layout.moved(here, offset, -1)), layout.count - 1)
        out_ref[0] = orbitals_ref[0, q]
        out_ref[1] = orbitals_ref[1, q]
        for slot, ref in enumerate((potential_ref,) + tuple(others)):
            out_ref[2 + slot] = ref[...]


def total(parts):
    return jnp.sum(parts, axis=(0, 1), keepdims=True)


def fold(product):
    return jnp.sum(product.reshape(-1, 8, product.shape[-1]), axis=0)


def solve_kernel(layout, *refs):
    near, far, across = (layout.near, layout.far, layout.across)
    orbitals_ref, potential_ref = refs[:2]
    refs = refs[2:]
    pots, refs = (refs[: len(across)], refs[len(across) :])
    near_refs, refs = (refs[: len(near) - 1], refs[len(near) - 1 :])
    far_refs, refs = (refs[: len(far)], refs[len(far) :])
    outs, scratch = (refs[: len(near)], refs[len(near) :])
    diag, inv, padded_d, padded_h, evolved, res, shadow, direc, image, second = scratch
    bx, by, nz = potential_ref.shape
    nx, ny = (bx * layout.rows, by * layout.columns)
    here = layout.here()

    def corner(offset):
        a, s, c = layout.moved(here, offset)
        return a * bx, pl.multiple_of((s * layout.width + c) * by, 8)

    zero_edge = jnp.zeros((2, 2, ny + 2 * MARGIN, nz), jnp.float32)
    for padded in (padded_d, padded_h):
        padded[:, 0:2] = zero_edge
        padded[:, nx + 2 : nx + 4] = zero_edge
        padded[:, :, 0:MARGIN] = jnp.zeros((2, nx + 4, MARGIN, nz), jnp.float32)
        padded[:, :, ny + MARGIN : ny + 2 * MARGIN] = jnp.zeros((2, nx + 4, MARGIN, nz), jnp.float32)

    def place_orbital(offset, part, block):
        x0, y0 = corner(offset)
        padded_d[part, pl.ds(x0 + 2, bx), pl.ds(y0 + MARGIN, by), :] = block
        evolved[part, pl.ds(x0, bx), pl.ds(y0, by), :] = block

    def place_potential(offset, block):
        x0, y0 = corner(offset)
        d = HALF_STEP * (DIAGONAL + block)
        diag[pl.ds(x0, bx), pl.ds(y0, by), :] = d
        inv[pl.ds(x0, bx), pl.ds(y0, by), :] = K2 / (1.0 + d * d)

    mine = jnp.minimum(layout.solved_by(here), layout.count - 1)
    place_potential(near[0], potential_ref[...])
    for offset, ref in zip(across, pots):
        place_potential(offset, ref[...])
    for part in range(2):
        place_orbital(near[0], part, orbitals_ref[part, mine])
    for (da, _, dc), ref in zip(near[1:], near_refs):
        for ds in range(layout.segments):
            place_potential((da, ds, dc), ref[2 + ds])
        for part in range(2):
            place_orbital((da, 0, dc), part, ref[part])
    for offset, ref in zip(far, far_refs):
        for part in range(2):
            place_orbital(offset, part, ref[part])

    lane = lax.broadcasted_iota(jnp.int32, (ny, nz), 1)
    keep = {s: (lane >= s if s > 0 else lane < nz + s) for s in (1, -1, 2, -2)}

    def shifted(center, s):
        return jnp.where(keep[s], pltpu.roll(center, s % nz, 1), 0.0)

    def stencil(padded, part, x):
        center = padded[part, x + 2, MARGIN : MARGIN + ny, :]

        def ring(s):
            return (
                (padded[part, x + 2 + s, MARGIN : MARGIN + ny, :] + padded[part, x + 2 - s, MARGIN : MARGIN + ny, :])
                + (padded[part, x + 2, MARGIN + s : MARGIN + s + ny, :] + padded[part, x + 2, MARGIN - s : MARGIN - s + ny, :])
                + (shifted(center, s) + shifted(center, -s))
            )

        return center, ring(2) - RATIO * ring(1)

    def sums(count):
        return tuple(jnp.zeros((8, nz), jnp.float32) for _ in range(count))

    def precondition_at(re, im, x):
        d, scale = (diag[x], inv[x])
        return (re + d * im) * scale, (im - d * re) * scale

    def start(x, acc):
        d = diag[x]
        center_re, off_re = stencil(padded_d, 0, x)
        center_im, off_im = stencil(padded_d, 1, x)
        re = 2.0 * (d * center_im + K2 * off_im)
        im = -2.0 * (d * center_re + K2 * off_re)
        shadow[0, x] = re
        shadow[1, x] = im
        hat_re, hat_im = precondition_at(re, im, x)
        padded_h[0, x + 2, MARGIN : MARGIN + ny, :] = hat_re
        padded_h[1, x + 2, MARGIN : MARGIN + ny, :] = hat_im
        return (acc[0] + fold(re * re + im * im),)

    (norm,) = lax.fori_loop(0, nx, start, sums(1), unroll=8)
    rho = (total(norm), jnp.zeros((1, 1), jnp.float32))
    residual, direction = (shadow, shadow)
    hat, other = (padded_h, padded_d)

    for iteration in range(ITERS):

        def image_at(x, acc):
            _, off_re = stencil(hat, 0, x)
            _, off_im = stencil(hat, 1, x)
            re = direction[0, x] - off_im
            im = direction[1, x] + off_re
            image[0, x] = re
            image[1, x] = im
            s_re, s_im = (shadow[0, x], shadow[1, x])
            return (acc[0] + fold(s_re * re + s_im * im), acc[1] + fold(s_re * im - s_im * re))

        acc = lax.fori_loop(0, nx, image_at, sums(2), unroll=8)
        sigma = (total(acc[0]), total(acc[1]))
        alpha = divide_complex(rho, sigma)

        def half_at(x, acc):
            i_re, i_im = (image[0, x], image[1, x])
            re = residual[0, x] - (alpha[0] * i_re - alpha[1] * i_im)
            im = residual[1, x] - (alpha[0] * i_im + alpha[1] * i_re)
            res[0, x] = re
            res[1, x] = im
            hat_re, hat_im = precondition_at(re, im, x)
            other[0, x + 2, MARGIN : MARGIN + ny, :] = hat_re
            other[1, x + 2, MARGIN : MARGIN + ny, :] = hat_im
            s_re, s_im = (shadow[0, x], shadow[1, x])
            return (acc[0] + fold(s_re * re + s_im * im), acc[1] + fold(s_re * im - s_im * re))

        acc = lax.fori_loop(0, nx, half_at, sums(2), unroll=4)
        shadow_half = (total(acc[0]), total(acc[1]))

        def second_at(x, acc):
            _, off_re = stencil(other, 0, x)
            _, off_im = stencil(other, 1, x)
            h_re, h_im = (res[0, x], res[1, x])
            re = h_re - off_im
            im = h_im + off_re
            second[0, x] = re
            second[1, x] = im
            s_re, s_im = (shadow[0, x], shadow[1, x])
            return (
                acc[0] + fold(re * h_re + im * h_im),
                acc[1] + fold(re * h_im - im * h_re),
                acc[2] + fold(re * re + im * im),
                acc[3] + fold(s_re * re + s_im * im),
                acc[4] + fold(s_re * im - s_im * re),
            )

        acc = lax.fori_loop(0, nx, second_at, sums(5), unroll=8)
        cross_re, cross_im, norm, ss_re, ss_im = [total(part) for part in acc]
        omega = (cross_re / norm, cross_im / norm)
        alpha_hat = (alpha[0] * (1.0 / K2), alpha[1] * (1.0 / K2))
        omega_hat = (omega[0] * (1.0 / K2), omega[1] * (1.0 / K2))

        def step_evolved(base, at_d, at_h):
            along_d = complex_mul(alpha_hat, at_d)
            along_h = complex_mul(omega_hat, at_h)
            return (base[0] + (along_d[0] + along_h[0]), base[1] + (along_d[1] + along_h[1]))

        if iteration + 1 < ITERS:
            moved = complex_mul(omega, (ss_re, ss_im))
            rho_next = (shadow_half[0] - moved[0], shadow_half[1] - moved[1])
            beta = complex_mul(divide_complex(rho_next, rho), divide_complex(alpha, omega))
            beta_omega = complex_mul(beta, omega)
            rho = rho_next

            def update_at(x, carry):
                at_d = (hat[0, x + 2, MARGIN : MARGIN + ny, :], hat[1, x + 2, MARGIN : MARGIN + ny, :])
                at_h = (other[0, x + 2, MARGIN : MARGIN + ny, :], other[1, x + 2, MARGIN : MARGIN + ny, :])
                e = step_evolved((evolved[0, x], evolved[1, x]), at_d, at_h)
                evolved[0, x] = e[0]
                evolved[1, x] = e[1]
                w = complex_mul(omega, (second[0, x], second[1, x]))
                r_re = res[0, x] - w[0]
                r_im = res[1, x] - w[1]
                res[0, x] = r_re
                res[1, x] = r_im
                p = complex_mul(beta, (direction[0, x], direction[1, x]))
                v = complex_mul(beta_omega, (image[0, x], image[1, x]))
                p_re = r_re + (p[0] - v[0])
                p_im = r_im + (p[1] - v[1])
                direc[0, x] = p_re
                direc[1, x] = p_im
                hat_re, hat_im = precondition_at(p_re, p_im, x)
                hat[0, x + 2, MARGIN : MARGIN + ny, :] = hat_re
                hat[1, x + 2, MARGIN : MARGIN + ny, :] = hat_im
                return carry

            lax.fori_loop(0, nx, update_at, 0, unroll=4)
            residual, direction = (res, direc)
        else:
            for offset, out in zip(near, outs):
                x0, y0 = corner(offset)

                def finish_at(i, carry):
                    x, y = (x0 + i, pl.ds(y0, by))
                    yp = pl.ds(y0 + MARGIN, by)
                    at_d = (hat[0, x + 2, yp, :], hat[1, x + 2, yp, :])
                    at_h = (other[0, x + 2, yp, :], other[1, x + 2, yp, :])
                    e = step_evolved((evolved[0, x, y, :], evolved[1, x, y, :]), at_d, at_h)
                    w = complex_mul(omega, (second[0, x, y, :], second[1, x, y, :]))
                    out[0, i] = e[0]
                    out[1, i] = e[1]
                    out[2, i] = res[0, x, y, :] - w[0]
                    out[3, i] = res[1, x, y, :] - w[1]
                    return carry

                lax.fori_loop(0, bx, finish_at, 0)


def unpack_kernel(layout, *refs):
    blocks, (evolved_ref, residual_ref) = (refs[: len(layout.near)], refs[len(layout.near) :])
    here = layout.here()
    for offset, block in zip(layout.near, blocks):
        q = layout.solved_by(layout.moved(here, offset, -1))

        @pl.when(q < layout.count)
        def _():
            for part in range(2):
                evolved_ref[part, q] = block[part]
                residual_ref[part, q] = block[2 + part]


VMEM_SPEC = pl.BlockSpec(memory_space=pltpu.VMEM)


def whole_call(kernel, operands, out_shapes, limit, scratch=()):
    return pl.pallas_call(
        kernel,
        out_shape=[jax.ShapeDtypeStruct(dims, jnp.float32) for dims in out_shapes],
        in_specs=[VMEM_SPEC] * len(operands),
        out_specs=[VMEM_SPEC] * len(out_shapes),
        scratch_shapes=list(scratch),
        compiler_params=pltpu.CompilerParams(vmem_limit_bytes=limit),
    )(*operands)


def solve_scratch(nx, ny, nz):
    field = pltpu.VMEM((2, nx, ny, nz), jnp.float32)
    padded = pltpu.VMEM((2, nx + 4, ny + 2 * MARGIN, nz), jnp.float32)
    scalar_field = pltpu.VMEM((nx, ny, nz), jnp.float32)
    return [scalar_field] * 2 + [padded] * 2 + [field] * 6


def gathered(layout, orbitals, potential):
    _, _, bx, by, nz = orbitals.shape
    axes = ("orb", "gx", "gyz")
    near, far, across = (layout.near, layout.far, layout.across)
    slots = 2 + layout.segments

    def fetch(array, offset, to_owner):
        return lax.ppermute(array, axes, layout.pairs(offset, False, to_owner))

    pots = [fetch(potential, offset, None) for offset in across]
    far_messages = whole_call(
        functools.partial(pack_far_kernel, layout),
        [orbitals],
        [(2, bx, by, nz)] * len(far),
        4 * 2**20,
    )
    far_blocks = [fetch(message, offset, True) for offset, message in zip(far, far_messages)]
    near_messages = whole_call(
        functools.partial(pack_near_kernel, layout),
        [orbitals, potential] + pots,
        [(slots, bx, by, nz)] * (len(near) - 1),
        4 * 2**20,
    )
    near_blocks = [fetch(message, offset, True) for offset, message in zip(near[1:], near_messages)]
    pieces = whole_call(
        functools.partial(solve_kernel, layout),
        [orbitals, potential] + pots + near_blocks + far_blocks,
        [(4, bx, by, nz)] * len(near),
        28 * 2**20,
        solve_scratch(bx * layout.rows, by * layout.columns, nz),
    )
    arrived = [pieces[0]]
    for offset, piece in zip(near[1:], pieces[1:]):
        arrived.append(lax.ppermute(piece, axes, layout.pairs(offset, True, False)))
    return whole_call(
        functools.partial(unpack_kernel, layout), arrived, [orbitals.shape] * 2, 6 * 2**20
    )


def solution(mesh):
    sizes = dict(mesh.shape)

    def shards(orbitals, potential):
        _, count, bx, by, nz = orbitals.shape
        layout = Layout(sizes["orb"], sizes["gx"], sizes["gyz"], count)
        nx, ny = (bx * layout.rows, by * layout.columns)
        fields = 24 * 4 * (nx + 4) * (ny + 2 * MARGIN) * nz
        if layout.fits and fields <= WORKING_SET and by % 8 == 0 and nz % 128 == 0:
            return tuple(gathered(layout, orbitals, potential))
        return distributed(orbitals, potential)

    return jax.shard_map(
        shards,
        mesh=mesh,
        in_specs=(P(None, "orb", "gx", "gyz", None), P("gx", "gyz", None)),
        out_specs=(P(None, "orb", "gx", "gyz", None), P(None, "orb", "gx", "gyz", None)),
        check_vma=False,
    )
```

```python
import functools

import jax
import jax.numpy as jnp
from jax import lax
from jax.experimental import pallas as pl
from jax.experimental.pallas import tpu as pltpu
from jax.sharding import PartitionSpec as P


ITERS = 4


SPACING = 0.25
HALF_STEP = 0.05
COEFF_NEAR = 4.0 / 3.0
COEFF_FAR = -1.0 / 12.0
COEFF_SELF = -2.5

RATIO = -COEFF_NEAR / COEFF_FAR
K2 = HALF_STEP * -0.5 / SPACING**2 * COEFF_FAR
DIAGONAL = -0.5 / SPACING**2 * 3.0 * COEFF_SELF
MARGIN = 8
WORKING_SET = 40 * 2**20


def with_halo(array, sides, width):
    for axis, dim in sides:
        size, length = (lax.axis_size(axis), array.shape[dim])
        up = [(i, (i + 1) % size) for i in range(size - 1)]
        down = [(j, i) for i, j in up]
        last = lax.slice_in_dim(array, length - width, length, axis=dim)
        leading = lax.slice_in_dim(array, 0, width, axis=dim)
        before = lax.ppermute(last, axis, up)
        after = lax.ppermute(leading, axis, down)
        array = jnp.concatenate([before, array, after], axis=dim)
    return array


def laplace_apply(padded, potential):
    extent = (padded.shape[2] - 4, padded.shape[3] - 4, padded.shape[4] - 4)

    def window(shift_x, shift_y, shift_z):
        return padded[
            :,
            :,
            2 + shift_x : 2 + shift_x + extent[0],
            2 + shift_y : 2 + shift_y + extent[1],
            2 + shift_z : 2 + shift_z + extent[2],
        ]

    center = window(0, 0, 0)
    summed = 3.0 * COEFF_SELF * center
    for offset, weight in ((1, COEFF_NEAR), (2, COEFF_FAR)):
        summed = summed + weight * (
            window(offset, 0, 0)
            + window(-offset, 0, 0)
            + window(0, offset, 0)
            + window(0, -offset, 0)
            + window(0, 0, offset)
            + window(0, 0, -offset)
        )
    return -0.5 / SPACING**2 * summed + potential * center


def pad_depth(vector):
    return jnp.pad(vector, ((0, 0), (0, 0), (0, 0), (0, 0), (2, 2)))


def system(vector, applied):
    return jnp.stack([vector[0] - HALF_STEP * applied[1], vector[1] + HALF_STEP * applied[0]])


def precondition(vector, potential):
    diagonal = HALF_STEP * (3.75 / SPACING**2 + potential)
    divisor = 1.0 + diagonal * diagonal
    return jnp.stack(
        [(vector[0] + diagonal * vector[1]) / divisor, (vector[1] - diagonal * vector[0]) / divisor]
    )


def braket(left, right):
    real_part = jnp.sum(left[0] * right[0] + left[1] * right[1], axis=(1, 2, 3))
    imag_part = jnp.sum(left[0] * right[1] - left[1] * right[0], axis=(1, 2, 3))
    return (real_part, imag_part)


def times_complex(first, second):
    return (
        first[0] * second[0] - first[1] * second[1],
        first[0] * second[1] + first[1] * second[0],
    )


def divide_complex(first, second):
    modulus = second[0] * second[0] + second[1] * second[1]
    return (
        (first[0] * second[0] + first[1] * second[1]) / modulus,
        (first[1] * second[0] - first[0] * second[1]) / modulus,
    )


def scale_complex(coeff, vector):
    real_coef = coeff[0][:, None, None, None]
    imag_coef = coeff[1][:, None, None, None]
    return jnp.stack(
        [
            real_coef * vector[0] - imag_coef * vector[1],
            real_coef * vector[1] + imag_coef * vector[0],
        ]
    )


def distributed(orbitals, potential):
    def apply_shallow(vector):
        padded = with_halo(vector, (("gx", 2), ("gyz", 3)), 2)
        return laplace_apply(pad_depth(padded), potential)

    h_orbitals = apply_shallow(orbitals)
    residual = jnp.stack([2.0 * HALF_STEP * h_orbitals[1], -2.0 * HALF_STEP * h_orbitals[0]])
    evolved = orbitals
    shadow = residual
    direction = residual
    rho_now = lax.psum(braket(shadow, residual), ("gx", "gyz"))
    for iteration in range(ITERS):
        dir_hat = precondition(direction, potential)
        image = system(dir_hat, apply_shallow(dir_hat))
        alpha_step = divide_complex(rho_now, lax.psum(braket(shadow, image), ("gx", "gyz")))
        half_step = residual - scale_complex(alpha_step, image)
        half_hat = precondition(half_step, potential)
        second = system(half_hat, apply_shallow(half_hat))
        cross_local = braket(second, half_step)
        norm_local = jnp.sum(second * second, axis=(0, 2, 3, 4))
        shadow_half = braket(shadow, half_step)
        shadow_second = braket(shadow, second)
        summed = lax.psum(
            (
                cross_local[0],
                cross_local[1],
                norm_local,
                shadow_half[0],
                shadow_half[1],
                shadow_second[0],
                shadow_second[1],
            ),
            ("gx", "gyz"),
        )
        cross_real, cross_imag, norm_second = (summed[0], summed[1], summed[2])
        omega_step = (cross_real / norm_second, cross_imag / norm_second)
        evolved = evolved + scale_complex(alpha_step, dir_hat) + scale_complex(omega_step, half_hat)
        residual = half_step - scale_complex(omega_step, second)
        if iteration + 1 < ITERS:
            along_second = times_complex(omega_step, (summed[5], summed[6]))
            rho_next = (summed[3] - along_second[0], summed[4] - along_second[1])
            beta_step = times_complex(
                divide_complex(rho_next, rho_now), divide_complex(alpha_step, omega_step)
            )
            direction = residual + scale_complex(
                beta_step, direction - scale_complex(omega_step, image)
            )
            rho_now = rho_next
    return (evolved, residual)


class Layout:
    def __init__(self, groups, rows, columns, count):
        self.groups, self.rows, self.columns, self.count = groups, rows, columns, count
        self.width = -(-count // rows)
        self.segments = columns // self.width
        self.fits = columns % self.width == 0
        inner = [(da, dc) for da in range(rows) for dc in range(self.width)]
        self.near = [(da, 0, dc) for da, dc in inner]
        self.far = [(da, ds, dc) for ds in range(1, self.segments) for da, dc in inner]
        self.across = [(0, ds, 0) for ds in range(1, self.segments)]

    def here(self):
        b = lax.axis_index("gyz")
        return lax.axis_index("gx"), b // self.width, lax.rem(b, self.width)

    def solved_by(self, place):
        q = self.solves(place)
        return jnp.where(lax.rem(lax.axis_index("orb"), 2) == 0, q, self.rows * self.width - 1 - q)

    def moved(self, place, offset, sign=1):
        sizes = (self.rows, self.segments, self.width)
        return tuple(
            p if o == 0 else lax.rem(p + (o if sign > 0 else n - o), n)
            for p, o, n in zip(place, offset, sizes)
        )

    def solves(self, place):
        row = place[0] + place[1]
        row = row % self.rows if isinstance(row, int) else lax.rem(row, self.rows)
        return row * self.width + place[2]

    def owned(self, group, place):
        q = self.solves(place)
        return q if group % 2 == 0 else self.rows * self.width - 1 - q

    def deliveries(self):
        places = [(a, b) for a in range(self.rows) for b in range(self.columns)]
        classes = {}
        for parity in range(2):
            owner = {p: self.owned(parity, (p[0], p[1] // self.width, p[1] % self.width)) for p in places}
            for target in places:
                for q in range(self.count):
                    if owner[target] == q:
                        continue
                    hops = lambda p: abs(p[0] - target[0]) + abs(p[1] - target[1])
                    source = min((p for p in places if owner[p] == q), key=hops)
                    step = (target[0] != source[0], target[1] - source[1])
                    classes.setdefault(step, []).append((parity, source, target, q))
        rounds = []
        for step in sorted(classes, key=lambda s: (-int(s[0]) - abs(s[1]), s)):
            for r in rounds:
                busy = {(m[0], m[1], 0) for m in r} | {(m[0], m[2], 1) for m in r}
                if not any((m[0], m[1], 0) in busy or (m[0], m[2], 1) in busy for m in classes[step]):
                    r += classes[step]
                    break
            else:
                rounds.append(list(classes[step]))
        return rounds

    def looked_up(self, entries):
        parity = lax.rem(lax.axis_index("orb"), 2)
        index = (parity * self.rows + lax.axis_index("gx")) * self.columns + lax.axis_index("gyz")
        value = jnp.int32(-1)
        for (p, (a, b)), entry in entries.items():
            value = jnp.where(index == (p * self.rows + a) * self.columns + b, entry, value)
        return value

    def pairs(self, offset, to_owner):
        found = []
        for g in range(self.groups):
            for a in range(self.rows):
                for b in range(self.columns):
                    place = (a, b // self.width, b % self.width)
                    sizes = (self.rows, self.segments, self.width)
                    other = tuple((p + o) % n for p, o, n in zip(place, offset, sizes))
                    source, target = (other, place)
                    if not to_owner or self.owned(g, target) < self.count:
                        found.append((self.linear(g, source), self.linear(g, target)))
        return found

    def linear(self, g, place):
        return (g * self.rows + place[0]) * self.columns + place[1] * self.width + place[2]


def complex_mul(first, second):
    return (
        first[0] * second[0] - first[1] * second[1],
        first[0] * second[1] + first[1] * second[0],
    )


def pack_far_kernel(layout, orbitals_ref, *out_refs):
    here = layout.here()
    for offset, out_ref in zip(layout.far, out_refs):
        q = jnp.minimum(layout.solved_by(layout.moved(here, offset, -1)), layout.count - 1)
        out_ref[0] = orbitals_ref[0, q]
        out_ref[1] = orbitals_ref[1, q]


def pack_near_kernel(layout, orbitals_ref, potential_ref, *refs):
    others, out_refs = (refs[: len(layout.across)], refs[len(layout.across) :])
    here = layout.here()
    for offset, out_ref in zip(layout.near[1:], out_refs):
        q = jnp.minimum(layout.solved_by(layout.moved(here, offset, -1)), layout.count - 1)
        out_ref[0] = orbitals_ref[0, q]
        out_ref[1] = orbitals_ref[1, q]
        for slot, ref in enumerate((potential_ref,) + tuple(others)):
            out_ref[2 + slot] = ref[...]


def total(parts):
    return jnp.sum(parts, axis=(0, 1), keepdims=True)


def fold(product):
    return jnp.sum(product.reshape(-1, 8, product.shape[-1]), axis=0)


def solve_kernel(layout, *refs):
    near, far, across = (layout.near, layout.far, layout.across)
    orbitals_ref, potential_ref = refs[:2]
    refs = refs[2:]
    pots, refs = (refs[: len(across)], refs[len(across) :])
    near_refs, refs = (refs[: len(near) - 1], refs[len(near) - 1 :])
    far_refs, refs = (refs[: len(far)], refs[len(far) :])
    rounds = layout.deliveries()
    outs, scratch = (refs[: 1 + len(rounds)], refs[1 + len(rounds) :])
    diag, inv, padded_d, padded_h, evolved, res, shadow, direc, image, second = scratch
    bx, by, nz = potential_ref.shape
    nx, ny = (bx * layout.rows, by * layout.columns)
    here = layout.here()

    def corner(offset):
        a, s, c = layout.moved(here, offset)
        return a * bx, pl.multiple_of((s * layout.width + c) * by, 8)

    zero_edge = jnp.zeros((2, 2, ny + 2 * MARGIN, nz), jnp.float32)
    for padded in (padded_d, padded_h):
        padded[:, 0:2] = zero_edge
        padded[:, nx + 2 : nx + 4] = zero_edge
        padded[:, :, 0:MARGIN] = jnp.zeros((2, nx + 4, MARGIN, nz), jnp.float32)
        padded[:, :, ny + MARGIN : ny + 2 * MARGIN] = jnp.zeros((2, nx + 4, MARGIN, nz), jnp.float32)

    def place_orbital(offset, part, block):
        x0, y0 = corner(offset)
        padded_d[part, pl.ds(x0 + 2, bx), pl.ds(y0 + MARGIN, by), :] = block
        evolved[part, pl.ds(x0, bx), pl.ds(y0, by), :] = block

    def place_potential(offset, block):
        x0, y0 = corner(offset)
        d = HALF_STEP * (DIAGONAL + block)
        diag[pl.ds(x0, bx), pl.ds(y0, by), :] = d
        inv[pl.ds(x0, bx), pl.ds(y0, by), :] = K2 / (1.0 + d * d)

    mine = jnp.minimum(layout.solved_by(here), layout.count - 1)
    place_potential(near[0], potential_ref[...])
    for offset, ref in zip(across, pots):
        place_potential(offset, ref[...])
    for part in range(2):
        place_orbital(near[0], part, orbitals_ref[part, mine])
    for (da, _, dc), ref in zip(near[1:], near_refs):
        for ds in range(layout.segments):
            place_potential((da, ds, dc), ref[2 + ds])
        for part in range(2):
            place_orbital((da, 0, dc), part, ref[part])
    for offset, ref in zip(far, far_refs):
        for part in range(2):
            place_orbital(offset, part, ref[part])

    lane = lax.broadcasted_iota(jnp.int32, (ny, nz), 1)
    keep = {s: (lane >= s if s > 0 else lane < nz + s) for s in (1, -1, 2, -2)}

    def shifted(center, s):
        return jnp.where(keep[s], pltpu.roll(center, s % nz, 1), 0.0)

    def stencil(padded, part, x):
        center = padded[part, x + 2, MARGIN : MARGIN + ny, :]

        def ring(s):
            return (
                (padded[part, x + 2 + s, MARGIN : MARGIN + ny, :] + padded[part, x + 2 - s, MARGIN : MARGIN + ny, :])
                + (padded[part, x + 2, MARGIN + s : MARGIN + s + ny, :] + padded[part, x + 2, MARGIN - s : MARGIN - s + ny, :])
                + (shifted(center, s) + shifted(center, -s))
            )

        return center, ring(2) - RATIO * ring(1)

    def sums(count):
        return tuple(jnp.zeros((8, nz), jnp.float32) for _ in range(count))

    def precondition_at(re, im, x):
        d, scale = (diag[x], inv[x])
        return (re + d * im) * scale, (im - d * re) * scale

    def start(x, acc):
        d = diag[x]
        center_re, off_re = stencil(padded_d, 0, x)
        center_im, off_im = stencil(padded_d, 1, x)
        re = 2.0 * (d * center_im + K2 * off_im)
        im = -2.0 * (d * center_re + K2 * off_re)
        shadow[0, x] = re
        shadow[1, x] = im
        hat_re, hat_im = precondition_at(re, im, x)
        padded_h[0, x + 2, MARGIN : MARGIN + ny, :] = hat_re
        padded_h[1, x + 2, MARGIN : MARGIN + ny, :] = hat_im
        return (acc[0] + fold(re * re + im * im),)

    (norm,) = lax.fori_loop(0, nx, start, sums(1), unroll=8)
    rho = (total(norm), jnp.zeros((1, 1), jnp.float32))
    residual, direction = (shadow, shadow)
    hat, other = (padded_h, padded_d)

    for iteration in range(ITERS):

        def image_at(x, acc):
            _, off_re = stencil(hat, 0, x)
            _, off_im = stencil(hat, 1, x)
            re = direction[0, x] - off_im
            im = direction[1, x] + off_re
            image[0, x] = re
            image[1, x] = im
            s_re, s_im = (shadow[0, x], shadow[1, x])
            return (acc[0] + fold(s_re * re + s_im * im), acc[1] + fold(s_re * im - s_im * re))

        acc = lax.fori_loop(0, nx, image_at, sums(2), unroll=8)
        sigma = (total(acc[0]), total(acc[1]))
        alpha = divide_complex(rho, sigma)

        def half_at(x, acc):
            i_re, i_im = (image[0, x], image[1, x])
            re = residual[0, x] - (alpha[0] * i_re - alpha[1] * i_im)
            im = residual[1, x] - (alpha[0] * i_im + alpha[1] * i_re)
            res[0, x] = re
            res[1, x] = im
            hat_re, hat_im = precondition_at(re, im, x)
            other[0, x + 2, MARGIN : MARGIN + ny, :] = hat_re
            other[1, x + 2, MARGIN : MARGIN + ny, :] = hat_im
            s_re, s_im = (shadow[0, x], shadow[1, x])
            return (acc[0] + fold(s_re * re + s_im * im), acc[1] + fold(s_re * im - s_im * re))

        acc = lax.fori_loop(0, nx, half_at, sums(2), unroll=4)
        shadow_half = (total(acc[0]), total(acc[1]))

        def second_at(x, acc):
            _, off_re = stencil(other, 0, x)
            _, off_im = stencil(other, 1, x)
            h_re, h_im = (res[0, x], res[1, x])
            re = h_re - off_im
            im = h_im + off_re
            second[0, x] = re
            second[1, x] = im
            s_re, s_im = (shadow[0, x], shadow[1, x])
            return (
                acc[0] + fold(re * h_re + im * h_im),
                acc[1] + fold(re * h_im - im * h_re),
                acc[2] + fold(re * re + im * im),
                acc[3] + fold(s_re * re + s_im * im),
                acc[4] + fold(s_re * im - s_im * re),
            )

        acc = lax.fori_loop(0, nx, second_at, sums(5), unroll=8)
        cross_re, cross_im, norm, ss_re, ss_im = [total(part) for part in acc]
        omega = (cross_re / norm, cross_im / norm)
        alpha_hat = (alpha[0] * (1.0 / K2), alpha[1] * (1.0 / K2))
        omega_hat = (omega[0] * (1.0 / K2), omega[1] * (1.0 / K2))

        def step_evolved(base, at_d, at_h):
            along_d = complex_mul(alpha_hat, at_d)
            along_h = complex_mul(omega_hat, at_h)
            return (base[0] + (along_d[0] + along_h[0]), base[1] + (along_d[1] + along_h[1]))

        if iteration + 1 < ITERS:
            moved = complex_mul(omega, (ss_re, ss_im))
            rho_next = (shadow_half[0] - moved[0], shadow_half[1] - moved[1])
            beta = complex_mul(divide_complex(rho_next, rho), divide_complex(alpha, omega))
            beta_omega = complex_mul(beta, omega)
            rho = rho_next

            def update_at(x, carry):
                at_d = (hat[0, x + 2, MARGIN : MARGIN + ny, :], hat[1, x + 2, MARGIN : MARGIN + ny, :])
                at_h = (other[0, x + 2, MARGIN : MARGIN + ny, :], other[1, x + 2, MARGIN : MARGIN + ny, :])
                e = step_evolved((evolved[0, x], evolved[1, x]), at_d, at_h)
                evolved[0, x] = e[0]
                evolved[1, x] = e[1]
                w = complex_mul(omega, (second[0, x], second[1, x]))
                r_re = res[0, x] - w[0]
                r_im = res[1, x] - w[1]
                res[0, x] = r_re
                res[1, x] = r_im
                p = complex_mul(beta, (direction[0, x], direction[1, x]))
                v = complex_mul(beta_omega, (image[0, x], image[1, x]))
                p_re = r_re + (p[0] - v[0])
                p_im = r_im + (p[1] - v[1])
                direc[0, x] = p_re
                direc[1, x] = p_im
                hat_re, hat_im = precondition_at(p_re, p_im, x)
                hat[0, x + 2, MARGIN : MARGIN + ny, :] = hat_re
                hat[1, x + 2, MARGIN : MARGIN + ny, :] = hat_im
                return carry

            lax.fori_loop(0, nx, update_at, 0, unroll=4)
            residual, direction = (res, direc)
        else:
            own = lax.axis_index("gx") * layout.columns + lax.axis_index("gyz")
            targets = [own] + [
                layout.looked_up({(m[0], m[1]): m[2][0] * layout.columns + m[2][1] for m in r}) for r in rounds
            ]
            for target, out in zip(targets, outs):
                x0 = target // layout.columns * bx
                y0 = pl.multiple_of(lax.rem(target, layout.columns) * by, 8)

                def finish_at(i, carry):
                    x, y = (x0 + i, pl.ds(y0, by))
                    yp = pl.ds(y0 + MARGIN, by)
                    at_d = (hat[0, x + 2, yp, :], hat[1, x + 2, yp, :])
                    at_h = (other[0, x + 2, yp, :], other[1, x + 2, yp, :])
                    e = step_evolved((evolved[0, x, y, :], evolved[1, x, y, :]), at_d, at_h)
                    w = complex_mul(omega, (second[0, x, y, :], second[1, x, y, :]))
                    out[0, i] = e[0]
                    out[1, i] = e[1]
                    out[2, i] = res[0, x, y, :] - w[0]
                    out[3, i] = res[1, x, y, :] - w[1]
                    return carry

                @pl.when(target >= 0)
                def _():
                    lax.fori_loop(0, bx, finish_at, 0, unroll=4)


def unpack_kernel(layout, *refs):
    rounds = layout.deliveries()
    blocks, (evolved_ref, residual_ref) = (refs[: 1 + len(rounds)], refs[1 + len(rounds) :])
    mine = layout.solved_by(layout.here())
    orbitals = [jnp.where(mine < layout.count, mine, -1)]
    orbitals += [layout.looked_up({(m[0], m[2]): m[3] for m in r}) for r in rounds]
    for q, block in zip(orbitals, blocks):

        @pl.when(q >= 0)
        def _():
            for part in range(2):
                evolved_ref[part, q] = block[part]
                residual_ref[part, q] = block[2 + part]


VMEM_SPEC = pl.BlockSpec(memory_space=pltpu.VMEM)


def whole_call(kernel, operands, out_shapes, limit, scratch=()):
    return pl.pallas_call(
        kernel,
        out_shape=[jax.ShapeDtypeStruct(dims, jnp.float32) for dims in out_shapes],
        in_specs=[VMEM_SPEC] * len(operands),
        out_specs=[VMEM_SPEC] * len(out_shapes),
        scratch_shapes=list(scratch),
        compiler_params=pltpu.CompilerParams(vmem_limit_bytes=limit),
    )(*operands)


def solve_scratch(nx, ny, nz):
    field = pltpu.VMEM((2, nx, ny, nz), jnp.float32)
    padded = pltpu.VMEM((2, nx + 4, ny + 2 * MARGIN, nz), jnp.float32)
    scalar_field = pltpu.VMEM((nx, ny, nz), jnp.float32)
    return [scalar_field] * 2 + [padded] * 2 + [field] * 6


def gathered(layout, orbitals, potential):
    _, _, bx, by, nz = orbitals.shape
    axes = ("orb", "gx", "gyz")
    near, far, across = (layout.near, layout.far, layout.across)
    slots = 2 + layout.segments

    def fetch(array, offset, to_owner):
        return lax.ppermute(array, axes, layout.pairs(offset, to_owner))

    pots = [fetch(potential, offset, False) for offset in across]
    far_messages = whole_call(
        functools.partial(pack_far_kernel, layout),
        [orbitals],
        [(2, bx, by, nz)] * len(far),
        4 * 2**20,
    )
    far_blocks = [fetch(message, offset, True) for offset, message in zip(far, far_messages)]
    near_messages = whole_call(
        functools.partial(pack_near_kernel, layout),
        [orbitals, potential] + pots,
        [(slots, bx, by, nz)] * (len(near) - 1),
        4 * 2**20,
    )
    near_blocks = [fetch(message, offset, True) for offset, message in zip(near[1:], near_messages)]
    rounds = layout.deliveries()
    pieces = whole_call(
        functools.partial(solve_kernel, layout),
        [orbitals, potential] + pots + near_blocks + far_blocks,
        [(4, bx, by, nz)] * (1 + len(rounds)),
        28 * 2**20,
        solve_scratch(bx * layout.rows, by * layout.columns, nz),
    )
    arrived = [pieces[0]]
    for messages, piece in zip(rounds, pieces[1:]):
        pairs = [
            ((g * layout.rows + s[0]) * layout.columns + s[1], (g * layout.rows + d[0]) * layout.columns + d[1])
            for g in range(layout.groups)
            for parity, s, d, _ in messages
            if g % 2 == parity
        ]
        arrived.append(lax.ppermute(piece, axes, pairs))
    return whole_call(
        functools.partial(unpack_kernel, layout), arrived, [orbitals.shape] * 2, 6 * 2**20
    )


def solution(mesh):
    sizes = dict(mesh.shape)

    def shards(orbitals, potential):
        _, count, bx, by, nz = orbitals.shape
        layout = Layout(sizes["orb"], sizes["gx"], sizes["gyz"], count)
        nx, ny = (bx * layout.rows, by * layout.columns)
        fields = 24 * 4 * (nx + 4) * (ny + 2 * MARGIN) * nz
        if layout.fits and fields <= WORKING_SET and by % 8 == 0 and nz % 128 == 0:
            return tuple(gathered(layout, orbitals, potential))
        return distributed(orbitals, potential)

    return jax.shard_map(
        shards,
        mesh=mesh,
        in_specs=(P(None, "orb", "gx", "gyz", None), P("gx", "gyz", None)),
        out_specs=(P(None, "orb", "gx", "gyz", None), P(None, "orb", "gx", "gyz", None)),
        check_vma=False,
    )
```

```python
import functools
import math

import jax
import jax.numpy as jnp
from jax import lax
from jax.experimental import pallas as pl
from jax.experimental.pallas import tpu as pltpu
from jax.sharding import PartitionSpec as P


ITERS = 4


SPACING = 0.25
HALF_STEP = 0.05
COEFF_NEAR = 4.0 / 3.0
COEFF_FAR = -1.0 / 12.0
COEFF_SELF = -2.5

RATIO = -COEFF_NEAR / COEFF_FAR
K2 = HALF_STEP * -0.5 / SPACING**2 * COEFF_FAR
DIAGONAL = -0.5 / SPACING**2 * 3.0 * COEFF_SELF
MARGIN = 8
PLANES = 32
WORKING_SET = 40 * 2**20


def with_halo(array, sides, width):
    for axis, dim in sides:
        size, length = (lax.axis_size(axis), array.shape[dim])
        up = [(i, (i + 1) % size) for i in range(size - 1)]
        down = [(j, i) for i, j in up]
        last = lax.slice_in_dim(array, length - width, length, axis=dim)
        leading = lax.slice_in_dim(array, 0, width, axis=dim)
        before = lax.ppermute(last, axis, up)
        after = lax.ppermute(leading, axis, down)
        array = jnp.concatenate([before, array, after], axis=dim)
    return array


def laplace_apply(padded, potential):
    extent = (padded.shape[2] - 4, padded.shape[3] - 4, padded.shape[4] - 4)

    def window(shift_x, shift_y, shift_z):
        return padded[
            :,
            :,
            2 + shift_x : 2 + shift_x + extent[0],
            2 + shift_y : 2 + shift_y + extent[1],
            2 + shift_z : 2 + shift_z + extent[2],
        ]

    center = window(0, 0, 0)
    summed = 3.0 * COEFF_SELF * center
    for offset, weight in ((1, COEFF_NEAR), (2, COEFF_FAR)):
        summed = summed + weight * (
            window(offset, 0, 0)
            + window(-offset, 0, 0)
            + window(0, offset, 0)
            + window(0, -offset, 0)
            + window(0, 0, offset)
            + window(0, 0, -offset)
        )
    return -0.5 / SPACING**2 * summed + potential * center


def pad_depth(vector):
    return jnp.pad(vector, ((0, 0), (0, 0), (0, 0), (0, 0), (2, 2)))


def system(vector, applied):
    return jnp.stack([vector[0] - HALF_STEP * applied[1], vector[1] + HALF_STEP * applied[0]])


def precondition(vector, potential):
    diagonal = HALF_STEP * (3.75 / SPACING**2 + potential)
    divisor = 1.0 + diagonal * diagonal
    return jnp.stack(
        [(vector[0] + diagonal * vector[1]) / divisor, (vector[1] - diagonal * vector[0]) / divisor]
    )


def braket(left, right):
    real_part = jnp.sum(left[0] * right[0] + left[1] * right[1], axis=(1, 2, 3))
    imag_part = jnp.sum(left[0] * right[1] - left[1] * right[0], axis=(1, 2, 3))
    return (real_part, imag_part)


def times_complex(first, second):
    return (
        first[0] * second[0] - first[1] * second[1],
        first[0] * second[1] + first[1] * second[0],
    )


def divide_complex(first, second):
    modulus = second[0] * second[0] + second[1] * second[1]
    return (
        (first[0] * second[0] + first[1] * second[1]) / modulus,
        (first[1] * second[0] - first[0] * second[1]) / modulus,
    )


def scale_complex(coeff, vector):
    real_coef = coeff[0][:, None, None, None]
    imag_coef = coeff[1][:, None, None, None]
    return jnp.stack(
        [
            real_coef * vector[0] - imag_coef * vector[1],
            real_coef * vector[1] + imag_coef * vector[0],
        ]
    )


def distributed(orbitals, potential):
    def apply_shallow(vector):
        padded = with_halo(vector, (("gx", 2), ("gyz", 3)), 2)
        return laplace_apply(pad_depth(padded), potential)

    h_orbitals = apply_shallow(orbitals)
    residual = jnp.stack([2.0 * HALF_STEP * h_orbitals[1], -2.0 * HALF_STEP * h_orbitals[0]])
    evolved = orbitals
    shadow = residual
    direction = residual
    rho_now = lax.psum(braket(shadow, residual), ("gx", "gyz"))
    for iteration in range(ITERS):
        dir_hat = precondition(direction, potential)
        image = system(dir_hat, apply_shallow(dir_hat))
        alpha_step = divide_complex(rho_now, lax.psum(braket(shadow, image), ("gx", "gyz")))
        half_step = residual - scale_complex(alpha_step, image)
        half_hat = precondition(half_step, potential)
        second = system(half_hat, apply_shallow(half_hat))
        cross_local = braket(second, half_step)
        norm_local = jnp.sum(second * second, axis=(0, 2, 3, 4))
        shadow_half = braket(shadow, half_step)
        shadow_second = braket(shadow, second)
        summed = lax.psum(
            (
                cross_local[0],
                cross_local[1],
                norm_local,
                shadow_half[0],
                shadow_half[1],
                shadow_second[0],
                shadow_second[1],
            ),
            ("gx", "gyz"),
        )
        cross_real, cross_imag, norm_second = (summed[0], summed[1], summed[2])
        omega_step = (cross_real / norm_second, cross_imag / norm_second)
        evolved = evolved + scale_complex(alpha_step, dir_hat) + scale_complex(omega_step, half_hat)
        residual = half_step - scale_complex(omega_step, second)
        if iteration + 1 < ITERS:
            along_second = times_complex(omega_step, (summed[5], summed[6]))
            rho_next = (summed[3] - along_second[0], summed[4] - along_second[1])
            beta_step = times_complex(
                divide_complex(rho_next, rho_now), divide_complex(alpha_step, omega_step)
            )
            direction = residual + scale_complex(
                beta_step, direction - scale_complex(omega_step, image)
            )
            rho_now = rho_next
    return (evolved, residual)


class Layout:
    def __init__(self, groups, rows, columns, count):
        self.groups, self.rows, self.columns, self.count = groups, rows, columns, count
        self.width = -(-count // rows)
        self.segments = columns // self.width
        self.fits = columns % self.width == 0
        inner = [(da, dc) for da in range(rows) for dc in range(self.width)]
        self.near = [(da, 0, dc) for da, dc in inner]
        self.far = [(da, ds, dc) for ds in range(1, self.segments) for da, dc in inner]
        self.across = [(0, ds, 0) for ds in range(1, self.segments)]

    def here(self):
        b = lax.axis_index("gyz")
        return lax.axis_index("gx"), b // self.width, lax.rem(b, self.width)

    def solved_by(self, place):
        q = self.solves(place)
        return jnp.where(lax.rem(lax.axis_index("orb"), 2) == 0, q, self.rows * self.width - 1 - q)

    def moved(self, place, offset, sign=1):
        sizes = (self.rows, self.segments, self.width)
        return tuple(
            p if o == 0 else lax.rem(p + (o if sign > 0 else n - o), n)
            for p, o, n in zip(place, offset, sizes)
        )

    def solves(self, place):
        row = place[0] + place[1]
        row = row % self.rows if isinstance(row, int) else lax.rem(row, self.rows)
        return row * self.width + place[2]

    def owned(self, group, place):
        q = self.solves(place)
        return q if group % 2 == 0 else self.rows * self.width - 1 - q

    def deliveries(self):
        places = [(a, b) for a in range(self.rows) for b in range(self.columns)]
        classes = {}
        for parity in range(2):
            owner = {p: self.owned(parity, (p[0], p[1] // self.width, p[1] % self.width)) for p in places}
            for target in places:
                for q in range(self.count):
                    if owner[target] == q:
                        continue
                    hops = lambda p: abs(p[0] - target[0]) + abs(p[1] - target[1])
                    source = min((p for p in places if owner[p] == q), key=hops)
                    step = (target[0] != source[0], target[1] - source[1])
                    classes.setdefault(step, []).append((parity, source, target, q))
        rounds = []
        for step in sorted(classes, key=lambda s: (-int(s[0]) - abs(s[1]), s)):
            for r in rounds:
                busy = {(m[0], m[1], 0) for m in r} | {(m[0], m[2], 1) for m in r}
                if not any((m[0], m[1], 0) in busy or (m[0], m[2], 1) in busy for m in classes[step]):
                    r += classes[step]
                    break
            else:
                rounds.append(list(classes[step]))
        return rounds

    def looked_up(self, entries):
        parity = lax.rem(lax.axis_index("orb"), 2)
        index = (parity * self.rows + lax.axis_index("gx")) * self.columns + lax.axis_index("gyz")
        value = jnp.int32(-1)
        for (p, (a, b)), entry in entries.items():
            value = jnp.where(index == (p * self.rows + a) * self.columns + b, entry, value)
        return value

    def pairs(self, offset, to_owner):
        found = []
        for g in range(self.groups):
            for a in range(self.rows):
                for b in range(self.columns):
                    place = (a, b // self.width, b % self.width)
                    sizes = (self.rows, self.segments, self.width)
                    other = tuple((p + o) % n for p, o, n in zip(place, offset, sizes))
                    source, target = (other, place)
                    if not to_owner or self.owned(g, target) < self.count:
                        found.append((self.linear(g, source), self.linear(g, target)))
        return found

    def linear(self, g, place):
        return (g * self.rows + place[0]) * self.columns + place[1] * self.width + place[2]


def complex_mul(first, second):
    return (
        first[0] * second[0] - first[1] * second[1],
        first[0] * second[1] + first[1] * second[0],
    )


def pack_far_kernel(layout, orbitals_ref, *out_refs):
    here = layout.here()
    for offset, out_ref in zip(layout.far, out_refs):
        q = jnp.minimum(layout.solved_by(layout.moved(here, offset, -1)), layout.count - 1)
        out_ref[0] = orbitals_ref[0, q]
        out_ref[1] = orbitals_ref[1, q]


def pack_near_kernel(layout, orbitals_ref, potential_ref, *refs):
    others, out_refs = (refs[: len(layout.across)], refs[len(layout.across) :])
    here = layout.here()
    for offset, out_ref in zip(layout.near[1:], out_refs):
        q = jnp.minimum(layout.solved_by(layout.moved(here, offset, -1)), layout.count - 1)
        out_ref[0] = orbitals_ref[0, q]
        out_ref[1] = orbitals_ref[1, q]
        for slot, ref in enumerate((potential_ref,) + tuple(others)):
            out_ref[2 + slot] = ref[...]


def total(parts):
    return jnp.sum(jnp.sum(parts, axis=0, keepdims=True), axis=1, keepdims=True)


def fold(product):
    return jnp.sum(product.reshape(-1, 8, product.shape[-1]), axis=0)


def solve_kernel(layout, *refs):
    near, far, across = (layout.near, layout.far, layout.across)
    orbitals_ref, potential_ref = refs[:2]
    refs = refs[2:]
    pots, refs = (refs[: len(across)], refs[len(across) :])
    near_refs, refs = (refs[: len(near) - 1], refs[len(near) - 1 :])
    far_refs, refs = (refs[: len(far)], refs[len(far) :])
    rounds = layout.deliveries()
    outs, scratch = (refs[: 1 + len(rounds)], refs[1 + len(rounds) :])
    diag, inv, padded_d, padded_h, evolved, res, shadow, direc, image, second = scratch
    bx, by, nz = potential_ref.shape
    nx, ny = (bx * layout.rows, by * layout.columns)
    planes = math.gcd(nx, PLANES)
    here = layout.here()

    def corner(offset):
        a, s, c = layout.moved(here, offset)
        return a * bx, pl.multiple_of((s * layout.width + c) * by, 8)

    zero_edge = jnp.zeros((2, 2, ny + 2 * MARGIN, nz), jnp.float32)
    for padded in (padded_d, padded_h):
        padded[:, 0:2] = zero_edge
        padded[:, nx + 2 : nx + 4] = zero_edge
        padded[:, :, 0:MARGIN] = jnp.zeros((2, nx + 4, MARGIN, nz), jnp.float32)
        padded[:, :, ny + MARGIN : ny + 2 * MARGIN] = jnp.zeros((2, nx + 4, MARGIN, nz), jnp.float32)

    def place_orbital(offset, part, block):
        x0, y0 = corner(offset)
        padded_d[part, pl.ds(x0 + 2, bx), pl.ds(y0 + MARGIN, by), :] = block
        evolved[part, pl.ds(x0, bx), pl.ds(y0, by), :] = block

    def place_potential(offset, block):
        x0, y0 = corner(offset)
        d = HALF_STEP * (DIAGONAL + block)
        diag[pl.ds(x0, bx), pl.ds(y0, by), :] = d
        inv[pl.ds(x0, bx), pl.ds(y0, by), :] = K2 / (1.0 + d * d)

    mine = jnp.minimum(layout.solved_by(here), layout.count - 1)
    place_potential(near[0], potential_ref[...])
    for offset, ref in zip(across, pots):
        place_potential(offset, ref[...])
    for part in range(2):
        place_orbital(near[0], part, orbitals_ref[part, mine])
    for (da, _, dc), ref in zip(near[1:], near_refs):
        for ds in range(layout.segments):
            place_potential((da, ds, dc), ref[2 + ds])
        for part in range(2):
            place_orbital((da, 0, dc), part, ref[part])
    for offset, ref in zip(far, far_refs):
        for part in range(2):
            place_orbital(offset, part, ref[part])

    apart = jnp.abs(lax.broadcasted_iota(jnp.int32, (2 * nz, nz), 0) % nz - lax.broadcasted_iota(jnp.int32, (2 * nz, nz), 1))
    weights = jnp.where(apart == 1, -RATIO, jnp.where(apart == 2, 1.0, 0.0)).astype(jnp.bfloat16)

    def along_z(center):
        high = center.astype(jnp.bfloat16)
        low = (center - high.astype(jnp.float32)).astype(jnp.bfloat16)
        return jnp.dot(jnp.concatenate([high, low], axis=1), weights, preferred_element_type=jnp.float32)

    def stencils(padded, x):
        rows = pl.ds(MARGIN, ny)
        flat = [padded[part, pl.ds(x + 2, planes), rows, :].reshape(planes * ny, nz) for part in range(2)]
        deep = along_z(jnp.concatenate(flat, axis=0))

        def at(part, i):
            def ring(s):
                return (padded[part, x + i + 2 + s, rows, :] + padded[part, x + i + 2 - s, rows, :]) + (
                    padded[part, x + i + 2, MARGIN + s : MARGIN + s + ny, :]
                    + padded[part, x + i + 2, MARGIN - s : MARGIN - s + ny, :]
                )

            start = (part * planes + i) * ny
            return (ring(2) - RATIO * ring(1)) + deep[start : start + ny]

        return [[at(part, i) for i in range(planes)] for part in range(2)]

    def over_planes(padded, at, acc):
        def step(i, acc):
            base = i * planes
            re, im = stencils(padded, base)
            for k in range(planes):
                acc = at(base + k, re[k], im[k], acc)
            return acc

        return lax.fori_loop(0, nx // planes, step, acc)

    def sums(count):
        return tuple(jnp.zeros((8, nz), jnp.float32) for _ in range(count))

    def precondition_at(re, im, x):
        d, scale = (diag[x], inv[x])
        return (re + d * im) * scale, (im - d * re) * scale

    def start(x, off_re, off_im, acc):
        d = diag[x]
        center_re = padded_d[0, x + 2, MARGIN : MARGIN + ny, :]
        center_im = padded_d[1, x + 2, MARGIN : MARGIN + ny, :]
        re = 2.0 * (d * center_im + K2 * off_im)
        im = -2.0 * (d * center_re + K2 * off_re)
        shadow[0, x] = re
        shadow[1, x] = im
        hat_re, hat_im = precondition_at(re, im, x)
        padded_h[0, x + 2, MARGIN : MARGIN + ny, :] = hat_re
        padded_h[1, x + 2, MARGIN : MARGIN + ny, :] = hat_im
        return (acc[0] + fold(re * re + im * im),)

    (norm,) = over_planes(padded_d, start, sums(1))
    rho = (total(norm), jnp.zeros((1, 1), jnp.float32))
    residual, direction = (shadow, shadow)
    hat, other = (padded_h, padded_d)

    for iteration in range(ITERS):

        def image_at(x, off_re, off_im, acc):
            re = direction[0, x] - off_im
            im = direction[1, x] + off_re
            image[0, x] = re
            image[1, x] = im
            s_re, s_im = (shadow[0, x], shadow[1, x])
            return (acc[0] + fold(s_re * re + s_im * im), acc[1] + fold(s_re * im - s_im * re))

        acc = over_planes(hat, image_at, sums(2))
        sigma = (total(acc[0]), total(acc[1]))
        alpha = divide_complex(rho, sigma)

        def half_at(x, acc):
            i_re, i_im = (image[0, x], image[1, x])
            re = residual[0, x] - (alpha[0] * i_re - alpha[1] * i_im)
            im = residual[1, x] - (alpha[0] * i_im + alpha[1] * i_re)
            res[0, x] = re
            res[1, x] = im
            hat_re, hat_im = precondition_at(re, im, x)
            other[0, x + 2, MARGIN : MARGIN + ny, :] = hat_re
            other[1, x + 2, MARGIN : MARGIN + ny, :] = hat_im
            s_re, s_im = (shadow[0, x], shadow[1, x])
            return (acc[0] + fold(s_re * re + s_im * im), acc[1] + fold(s_re * im - s_im * re))

        acc = lax.fori_loop(0, nx, half_at, sums(2), unroll=4)
        shadow_half = (total(acc[0]), total(acc[1]))

        def second_at(x, off_re, off_im, acc):
            h_re, h_im = (res[0, x], res[1, x])
            re = h_re - off_im
            im = h_im + off_re
            second[0, x] = re
            second[1, x] = im
            s_re, s_im = (shadow[0, x], shadow[1, x])
            return (
                acc[0] + fold(re * h_re + im * h_im),
                acc[1] + fold(re * h_im - im * h_re),
                acc[2] + fold(re * re + im * im),
                acc[3] + fold(s_re * re + s_im * im),
                acc[4] + fold(s_re * im - s_im * re),
            )

        acc = over_planes(other, second_at, sums(5))
        cross_re, cross_im, norm, ss_re, ss_im = [total(part) for part in acc]
        omega = (cross_re / norm, cross_im / norm)
        alpha_hat = (alpha[0] * (1.0 / K2), alpha[1] * (1.0 / K2))
        omega_hat = (omega[0] * (1.0 / K2), omega[1] * (1.0 / K2))

        def step_evolved(base, at_d, at_h):
            along_d = complex_mul(alpha_hat, at_d)
            along_h = complex_mul(omega_hat, at_h)
            return (base[0] + (along_d[0] + along_h[0]), base[1] + (along_d[1] + along_h[1]))

        if iteration + 1 < ITERS:
            moved = complex_mul(omega, (ss_re, ss_im))
            rho_next = (shadow_half[0] - moved[0], shadow_half[1] - moved[1])
            beta = complex_mul(divide_complex(rho_next, rho), divide_complex(alpha, omega))
            beta_omega = complex_mul(beta, omega)
            rho = rho_next

            def update_at(x, carry):
                at_d = (hat[0, x + 2, MARGIN : MARGIN + ny, :], hat[1, x + 2, MARGIN : MARGIN + ny, :])
                at_h = (other[0, x + 2, MARGIN : MARGIN + ny, :], other[1, x + 2, MARGIN : MARGIN + ny, :])
                e = step_evolved((evolved[0, x], evolved[1, x]), at_d, at_h)
                evolved[0, x] = e[0]
                evolved[1, x] = e[1]
                w = complex_mul(omega, (second[0, x], second[1, x]))
                r_re = res[0, x] - w[0]
                r_im = res[1, x] - w[1]
                res[0, x] = r_re
                res[1, x] = r_im
                p = complex_mul(beta, (direction[0, x], direction[1, x]))
                v = complex_mul(beta_omega, (image[0, x], image[1, x]))
                p_re = r_re + (p[0] - v[0])
                p_im = r_im + (p[1] - v[1])
                direc[0, x] = p_re
                direc[1, x] = p_im
                hat_re, hat_im = precondition_at(p_re, p_im, x)
                hat[0, x + 2, MARGIN : MARGIN + ny, :] = hat_re
                hat[1, x + 2, MARGIN : MARGIN + ny, :] = hat_im
                return carry

            lax.fori_loop(0, nx, update_at, 0, unroll=4)
            residual, direction = (res, direc)
        else:
            own = lax.axis_index("gx") * layout.columns + lax.axis_index("gyz")
            targets = [own] + [
                layout.looked_up({(m[0], m[1]): m[2][0] * layout.columns + m[2][1] for m in r}) for r in rounds
            ]
            for target, out in zip(targets, outs):
                x0 = target // layout.columns * bx
                y0 = pl.multiple_of(lax.rem(target, layout.columns) * by, 8)

                def finish_at(i, carry):
                    x, y = (x0 + i, pl.ds(y0, by))
                    yp = pl.ds(y0 + MARGIN, by)
                    at_d = (hat[0, x + 2, yp, :], hat[1, x + 2, yp, :])
                    at_h = (other[0, x + 2, yp, :], other[1, x + 2, yp, :])
                    e = step_evolved((evolved[0, x, y, :], evolved[1, x, y, :]), at_d, at_h)
                    w = complex_mul(omega, (second[0, x, y, :], second[1, x, y, :]))
                    out[0, i] = e[0]
                    out[1, i] = e[1]
                    out[2, i] = res[0, x, y, :] - w[0]
                    out[3, i] = res[1, x, y, :] - w[1]
                    return carry

                @pl.when(target >= 0)
                def _():
                    lax.fori_loop(0, bx, finish_at, 0, unroll=4)


def unpack_kernel(layout, *refs):
    rounds = layout.deliveries()
    blocks, (evolved_ref, residual_ref) = (refs[: 1 + len(rounds)], refs[1 + len(rounds) :])
    mine = layout.solved_by(layout.here())
    orbitals = [jnp.where(mine < layout.count, mine, -1)]
    orbitals += [layout.looked_up({(m[0], m[2]): m[3] for m in r}) for r in rounds]
    for q, block in zip(orbitals, blocks):

        @pl.when(q >= 0)
        def _():
            for part in range(2):
                evolved_ref[part, q] = block[part]
                residual_ref[part, q] = block[2 + part]


VMEM_SPEC = pl.BlockSpec(memory_space=pltpu.VMEM)


def whole_call(kernel, operands, out_shapes, limit, scratch=()):
    return pl.pallas_call(
        kernel,
        out_shape=[jax.ShapeDtypeStruct(dims, jnp.float32) for dims in out_shapes],
        in_specs=[VMEM_SPEC] * len(operands),
        out_specs=[VMEM_SPEC] * len(out_shapes),
        scratch_shapes=list(scratch),
        compiler_params=pltpu.CompilerParams(vmem_limit_bytes=limit),
    )(*operands)


def solve_scratch(nx, ny, nz):
    field = pltpu.VMEM((2, nx, ny, nz), jnp.float32)
    padded = pltpu.VMEM((2, nx + 4, ny + 2 * MARGIN, nz), jnp.float32)
    scalar_field = pltpu.VMEM((nx, ny, nz), jnp.float32)
    return [scalar_field] * 2 + [padded] * 2 + [field] * 6


def gathered(layout, orbitals, potential):
    _, _, bx, by, nz = orbitals.shape
    axes = ("orb", "gx", "gyz")
    near, far, across = (layout.near, layout.far, layout.across)
    slots = 2 + layout.segments

    def fetch(array, offset, to_owner):
        return lax.ppermute(array, axes, layout.pairs(offset, to_owner))

    pots = [fetch(potential, offset, False) for offset in across]
    far_messages = whole_call(
        functools.partial(pack_far_kernel, layout), [orbitals], [(2, bx, by, nz)] * len(far), 4 * 2**20
    )
    far_blocks = [fetch(message, offset, True) for offset, message in zip(far, far_messages)]
    near_messages = whole_call(
        functools.partial(pack_near_kernel, layout),
        [orbitals, potential] + pots,
        [(slots, bx, by, nz)] * (len(near) - 1),
        4 * 2**20,
    )
    near_blocks = [fetch(message, offset, True) for offset, message in zip(near[1:], near_messages)]
    rounds = layout.deliveries()
    pieces = whole_call(
        functools.partial(solve_kernel, layout),
        [orbitals, potential] + pots + near_blocks + far_blocks,
        [(4, bx, by, nz)] * (1 + len(rounds)),
        28 * 2**20,
        solve_scratch(bx * layout.rows, by * layout.columns, nz),
    )
    arrived = [pieces[0]]
    for messages, piece in zip(rounds, pieces[1:]):
        pairs = [
            ((g * layout.rows + s[0]) * layout.columns + s[1], (g * layout.rows + d[0]) * layout.columns + d[1])
            for g in range(layout.groups)
            for parity, s, d, _ in messages
            if g % 2 == parity
        ]
        arrived.append(lax.ppermute(piece, axes, pairs))
    return whole_call(functools.partial(unpack_kernel, layout), arrived, [orbitals.shape] * 2, 6 * 2**20)


def solution(mesh):
    sizes = dict(mesh.shape)

    def shards(orbitals, potential):
        _, count, bx, by, nz = orbitals.shape
        layout = Layout(sizes["orb"], sizes["gx"], sizes["gyz"], count)
        nx, ny = (bx * layout.rows, by * layout.columns)
        fields = 24 * 4 * (nx + 4) * (ny + 2 * MARGIN) * nz
        if layout.fits and fields <= WORKING_SET and by % 8 == 0 and nz % 128 == 0:
            return tuple(gathered(layout, orbitals, potential))
        return distributed(orbitals, potential)

    return jax.shard_map(
        shards,
        mesh=mesh,
        in_specs=(P(None, "orb", "gx", "gyz", None), P("gx", "gyz", None)),
        out_specs=(P(None, "orb", "gx", "gyz", None), P(None, "orb", "gx", "gyz", None)),
        check_vma=False,
    )
```

```python
import functools
import math

import jax
import jax.numpy as jnp
from jax import lax
from jax.experimental import pallas as pl
from jax.experimental.pallas import tpu as pltpu
from jax.sharding import PartitionSpec as P


ITERS = 4


SPACING = 0.25
HALF_STEP = 0.05
COEFF_NEAR = 4.0 / 3.0
COEFF_FAR = -1.0 / 12.0
COEFF_SELF = -2.5

RATIO = -COEFF_NEAR / COEFF_FAR
K2 = HALF_STEP * -0.5 / SPACING**2 * COEFF_FAR
DIAGONAL = -0.5 / SPACING**2 * 3.0 * COEFF_SELF
MARGIN = 8
PLANES = 32
WORKING_SET = 40 * 2**20


def with_halo(array, sides, width):
    for axis, dim in sides:
        size, length = (lax.axis_size(axis), array.shape[dim])
        up = [(i, (i + 1) % size) for i in range(size - 1)]
        down = [(j, i) for i, j in up]
        last = lax.slice_in_dim(array, length - width, length, axis=dim)
        leading = lax.slice_in_dim(array, 0, width, axis=dim)
        before = lax.ppermute(last, axis, up)
        after = lax.ppermute(leading, axis, down)
        array = jnp.concatenate([before, array, after], axis=dim)
    return array


def laplace_apply(padded, potential):
    extent = (padded.shape[2] - 4, padded.shape[3] - 4, padded.shape[4] - 4)

    def window(shift_x, shift_y, shift_z):
        return padded[
            :,
            :,
            2 + shift_x : 2 + shift_x + extent[0],
            2 + shift_y : 2 + shift_y + extent[1],
            2 + shift_z : 2 + shift_z + extent[2],
        ]

    center = window(0, 0, 0)
    summed = 3.0 * COEFF_SELF * center
    for offset, weight in ((1, COEFF_NEAR), (2, COEFF_FAR)):
        summed = summed + weight * (
            window(offset, 0, 0)
            + window(-offset, 0, 0)
            + window(0, offset, 0)
            + window(0, -offset, 0)
            + window(0, 0, offset)
            + window(0, 0, -offset)
        )
    return -0.5 / SPACING**2 * summed + potential * center


def pad_depth(vector):
    return jnp.pad(vector, ((0, 0), (0, 0), (0, 0), (0, 0), (2, 2)))


def system(vector, applied):
    return jnp.stack([vector[0] - HALF_STEP * applied[1], vector[1] + HALF_STEP * applied[0]])


def precondition(vector, potential):
    diagonal = HALF_STEP * (3.75 / SPACING**2 + potential)
    divisor = 1.0 + diagonal * diagonal
    return jnp.stack(
        [(vector[0] + diagonal * vector[1]) / divisor, (vector[1] - diagonal * vector[0]) / divisor]
    )


def braket(left, right):
    real_part = jnp.sum(left[0] * right[0] + left[1] * right[1], axis=(1, 2, 3))
    imag_part = jnp.sum(left[0] * right[1] - left[1] * right[0], axis=(1, 2, 3))
    return (real_part, imag_part)


def times_complex(first, second):
    return (
        first[0] * second[0] - first[1] * second[1],
        first[0] * second[1] + first[1] * second[0],
    )


def divide_complex(first, second):
    modulus = second[0] * second[0] + second[1] * second[1]
    return (
        (first[0] * second[0] + first[1] * second[1]) / modulus,
        (first[1] * second[0] - first[0] * second[1]) / modulus,
    )


def scale_complex(coeff, vector):
    real_coef = coeff[0][:, None, None, None]
    imag_coef = coeff[1][:, None, None, None]
    return jnp.stack(
        [
            real_coef * vector[0] - imag_coef * vector[1],
            real_coef * vector[1] + imag_coef * vector[0],
        ]
    )


def distributed(orbitals, potential):
    def apply_shallow(vector):
        padded = with_halo(vector, (("gx", 2), ("gyz", 3)), 2)
        return laplace_apply(pad_depth(padded), potential)

    h_orbitals = apply_shallow(orbitals)
    residual = jnp.stack([2.0 * HALF_STEP * h_orbitals[1], -2.0 * HALF_STEP * h_orbitals[0]])
    evolved = orbitals
    shadow = residual
    direction = residual
    rho_now = lax.psum(braket(shadow, residual), ("gx", "gyz"))
    for iteration in range(ITERS):
        dir_hat = precondition(direction, potential)
        image = system(dir_hat, apply_shallow(dir_hat))
        alpha_step = divide_complex(rho_now, lax.psum(braket(shadow, image), ("gx", "gyz")))
        half_step = residual - scale_complex(alpha_step, image)
        half_hat = precondition(half_step, potential)
        second = system(half_hat, apply_shallow(half_hat))
        cross_local = braket(second, half_step)
        norm_local = jnp.sum(second * second, axis=(0, 2, 3, 4))
        shadow_half = braket(shadow, half_step)
        shadow_second = braket(shadow, second)
        summed = lax.psum(
            (
                cross_local[0],
                cross_local[1],
                norm_local,
                shadow_half[0],
                shadow_half[1],
                shadow_second[0],
                shadow_second[1],
            ),
            ("gx", "gyz"),
        )
        cross_real, cross_imag, norm_second = (summed[0], summed[1], summed[2])
        omega_step = (cross_real / norm_second, cross_imag / norm_second)
        evolved = evolved + scale_complex(alpha_step, dir_hat) + scale_complex(omega_step, half_hat)
        residual = half_step - scale_complex(omega_step, second)
        if iteration + 1 < ITERS:
            along_second = times_complex(omega_step, (summed[5], summed[6]))
            rho_next = (summed[3] - along_second[0], summed[4] - along_second[1])
            beta_step = times_complex(
                divide_complex(rho_next, rho_now), divide_complex(alpha_step, omega_step)
            )
            direction = residual + scale_complex(
                beta_step, direction - scale_complex(omega_step, image)
            )
            rho_now = rho_next
    return (evolved, residual)


class Layout:
    def __init__(self, groups, rows, columns, count):
        self.groups, self.rows, self.columns, self.count = groups, rows, columns, count
        self.width = -(-count // rows)
        self.segments = columns // self.width
        self.fits = columns % self.width == 0
        inner = [(da, dc) for da in range(rows) for dc in range(self.width)]
        self.near = [(da, 0, dc) for da, dc in inner]
        self.far = [(da, ds, dc) for ds in range(1, self.segments) for da, dc in inner]
        self.across = [(0, ds, 0) for ds in range(1, self.segments)]

    def here(self):
        b = lax.axis_index("gyz")
        return lax.axis_index("gx"), b // self.width, lax.rem(b, self.width)

    def solved_by(self, place):
        q = self.solves(place)
        return jnp.where(lax.rem(lax.axis_index("orb"), 2) == 0, q, self.rows * self.width - 1 - q)

    def moved(self, place, offset, sign=1):
        sizes = (self.rows, self.segments, self.width)
        return tuple(
            p if o == 0 else lax.rem(p + (o if sign > 0 else n - o), n)
            for p, o, n in zip(place, offset, sizes)
        )

    def solves(self, place):
        row = place[0] + place[1]
        row = row % self.rows if isinstance(row, int) else lax.rem(row, self.rows)
        return row * self.width + place[2]

    def owned(self, group, place):
        q = self.solves(place)
        return q if group % 2 == 0 else self.rows * self.width - 1 - q

    def deliveries(self):
        places = [(a, b) for a in range(self.rows) for b in range(self.columns)]
        classes = {}
        for parity in range(2):
            owner = {p: self.owned(parity, (p[0], p[1] // self.width, p[1] % self.width)) for p in places}
            for target in places:
                for q in range(self.count):
                    if owner[target] == q:
                        continue
                    hops = lambda p: abs(p[0] - target[0]) + abs(p[1] - target[1])
                    source = min((p for p in places if owner[p] == q), key=hops)
                    swap = min(target[1], source[1]) % 2 if target[0] == source[0] else 0
                    step = (target[0] != source[0], abs(target[1] - source[1]), swap)
                    classes.setdefault(step, []).append((parity, source, target, q))
        rounds = []
        for step in sorted(classes, key=lambda s: (s[2], s[0], -s[1])):
            for r in rounds:
                busy = {(m[0], m[1], 0) for m in r} | {(m[0], m[2], 1) for m in r}
                if not any((m[0], m[1], 0) in busy or (m[0], m[2], 1) in busy for m in classes[step]):
                    r += classes[step]
                    break
            else:
                rounds.append(list(classes[step]))
        return rounds

    def looked_up(self, entries):
        parity = lax.rem(lax.axis_index("orb"), 2)
        index = (parity * self.rows + lax.axis_index("gx")) * self.columns + lax.axis_index("gyz")
        value = jnp.int32(-1)
        for (p, (a, b)), entry in entries.items():
            value = jnp.where(index == (p * self.rows + a) * self.columns + b, entry, value)
        return value

    def pairs(self, offset, to_owner):
        found = []
        for g in range(self.groups):
            for a in range(self.rows):
                for b in range(self.columns):
                    place = (a, b // self.width, b % self.width)
                    sizes = (self.rows, self.segments, self.width)
                    other = tuple((p + o) % n for p, o, n in zip(place, offset, sizes))
                    source, target = (other, place)
                    if not to_owner or self.owned(g, target) < self.count:
                        found.append((self.linear(g, source), self.linear(g, target)))
        return found

    def linear(self, g, place):
        return (g * self.rows + place[0]) * self.columns + place[1] * self.width + place[2]


def complex_mul(first, second):
    return (
        first[0] * second[0] - first[1] * second[1],
        first[0] * second[1] + first[1] * second[0],
    )


def pack_far_kernel(layout, orbitals_ref, *out_refs):
    here = layout.here()
    for offset, out_ref in zip(layout.far, out_refs):
        q = jnp.minimum(layout.solved_by(layout.moved(here, offset, -1)), layout.count - 1)
        out_ref[0] = orbitals_ref[0, q]
        out_ref[1] = orbitals_ref[1, q]


def pack_near_kernel(layout, orbitals_ref, potential_ref, *refs):
    others, out_refs = (refs[: len(layout.across)], refs[len(layout.across) :])
    here = layout.here()
    for offset, out_ref in zip(layout.near[1:], out_refs):
        q = jnp.minimum(layout.solved_by(layout.moved(here, offset, -1)), layout.count - 1)
        out_ref[0] = orbitals_ref[0, q]
        out_ref[1] = orbitals_ref[1, q]
        for slot, ref in enumerate((potential_ref,) + tuple(others)):
            out_ref[2 + slot] = ref[...]


def total(parts):
    return jnp.sum(jnp.sum(parts, axis=0, keepdims=True), axis=1, keepdims=True)


def fold(product):
    return jnp.sum(product.reshape(-1, 8, product.shape[-1]), axis=0)


def solve_kernel(layout, *refs):
    near, far, across = (layout.near, layout.far, layout.across)
    orbitals_ref, potential_ref = refs[:2]
    refs = refs[2:]
    pots, refs = (refs[: len(across)], refs[len(across) :])
    near_refs, refs = (refs[: len(near) - 1], refs[len(near) - 1 :])
    far_refs, refs = (refs[: len(far)], refs[len(far) :])
    rounds = layout.deliveries()
    outs, scratch = (refs[: 1 + len(rounds)], refs[1 + len(rounds) :])
    diag, inv, padded_d, padded_h, evolved, res, shadow, direc, image, second = scratch
    bx, by, nz = potential_ref.shape
    nx, ny = (bx * layout.rows, by * layout.columns)
    planes = math.gcd(nx, PLANES)
    here = layout.here()

    def corner(offset):
        a, s, c = layout.moved(here, offset)
        return a * bx, pl.multiple_of((s * layout.width + c) * by, 8)

    zero_edge = jnp.zeros((2, 2, ny + 2 * MARGIN, nz), jnp.float32)
    for padded in (padded_d, padded_h):
        padded[:, 0:2] = zero_edge
        padded[:, nx + 2 : nx + 4] = zero_edge
        padded[:, :, 0:MARGIN] = jnp.zeros((2, nx + 4, MARGIN, nz), jnp.float32)
        padded[:, :, ny + MARGIN : ny + 2 * MARGIN] = jnp.zeros((2, nx + 4, MARGIN, nz), jnp.float32)

    def place_orbital(offset, part, block):
        x0, y0 = corner(offset)
        padded_d[part, pl.ds(x0 + 2, bx), pl.ds(y0 + MARGIN, by), :] = block
        evolved[part, pl.ds(x0, bx), pl.ds(y0, by), :] = block

    def place_potential(offset, block):
        x0, y0 = corner(offset)
        d = HALF_STEP * (DIAGONAL + block)
        diag[pl.ds(x0, bx), pl.ds(y0, by), :] = d
        inv[pl.ds(x0, bx), pl.ds(y0, by), :] = K2 / (1.0 + d * d)

    mine = jnp.minimum(layout.solved_by(here), layout.count - 1)
    place_potential(near[0], potential_ref[...])
    for offset, ref in zip(across, pots):
        place_potential(offset, ref[...])
    for part in range(2):
        place_orbital(near[0], part, orbitals_ref[part, mine])
    for (da, _, dc), ref in zip(near[1:], near_refs):
        for ds in range(layout.segments):
            place_potential((da, ds, dc), ref[2 + ds])
        for part in range(2):
            place_orbital((da, 0, dc), part, ref[part])
    for offset, ref in zip(far, far_refs):
        for part in range(2):
            place_orbital(offset, part, ref[part])

    apart = jnp.abs(lax.broadcasted_iota(jnp.int32, (2 * nz, nz), 0) % nz - lax.broadcasted_iota(jnp.int32, (2 * nz, nz), 1))
    weights = jnp.where(apart == 1, -RATIO, jnp.where(apart == 2, 1.0, 0.0)).astype(jnp.bfloat16)

    def along_z(center):
        high = center.astype(jnp.bfloat16)
        low = (center - high.astype(jnp.float32)).astype(jnp.bfloat16)
        return jnp.dot(jnp.concatenate([high, low], axis=1), weights, preferred_element_type=jnp.float32)

    def stencils(padded, x):
        rows = pl.ds(MARGIN, ny)
        flat = [padded[part, pl.ds(x + 2, planes), rows, :].reshape(planes * ny, nz) for part in range(2)]
        deep = along_z(jnp.concatenate(flat, axis=0))

        def at(part, i):
            def ring(s):
                return (padded[part, x + i + 2 + s, rows, :] + padded[part, x + i + 2 - s, rows, :]) + (
                    padded[part, x + i + 2, MARGIN + s : MARGIN + s + ny, :]
                    + padded[part, x + i + 2, MARGIN - s : MARGIN - s + ny, :]
                )

            start = (part * planes + i) * ny
            return (ring(2) - RATIO * ring(1)) + deep[start : start + ny]

        return [[at(part, i) for i in range(planes)] for part in range(2)]

    def over_planes(padded, at, acc):
        def step(i, acc):
            base = i * planes
            re, im = stencils(padded, base)
            for k in range(planes):
                acc = at(base + k, re[k], im[k], acc)
            return acc

        return lax.fori_loop(0, nx // planes, step, acc)

    def sums(count):
        return tuple(jnp.zeros((8, nz), jnp.float32) for _ in range(count))

    def precondition_at(re, im, x):
        d, scale = (diag[x], inv[x])
        return (re + d * im) * scale, (im - d * re) * scale

    def start(x, off_re, off_im, acc):
        d = diag[x]
        center_re = padded_d[0, x + 2, MARGIN : MARGIN + ny, :]
        center_im = padded_d[1, x + 2, MARGIN : MARGIN + ny, :]
        re = 2.0 * (d * center_im + K2 * off_im)
        im = -2.0 * (d * center_re + K2 * off_re)
        shadow[0, x] = re
        shadow[1, x] = im
        hat_re, hat_im = precondition_at(re, im, x)
        padded_h[0, x + 2, MARGIN : MARGIN + ny, :] = hat_re
        padded_h[1, x + 2, MARGIN : MARGIN + ny, :] = hat_im
        return (acc[0] + fold(re * re + im * im),)

    (norm,) = over_planes(padded_d, start, sums(1))
    rho = (total(norm), jnp.zeros((1, 1), jnp.float32))
    residual, direction = (shadow, shadow)
    hat, other = (padded_h, padded_d)

    for iteration in range(ITERS):

        def image_at(x, off_re, off_im, acc):
            re = direction[0, x] - off_im
            im = direction[1, x] + off_re
            image[0, x] = re
            image[1, x] = im
            s_re, s_im = (shadow[0, x], shadow[1, x])
            return (acc[0] + fold(s_re * re + s_im * im), acc[1] + fold(s_re * im - s_im * re))

        acc = over_planes(hat, image_at, sums(2))
        sigma = (total(acc[0]), total(acc[1]))
        alpha = divide_complex(rho, sigma)

        def half_at(x, acc):
            i_re, i_im = (image[0, x], image[1, x])
            re = residual[0, x] - (alpha[0] * i_re - alpha[1] * i_im)
            im = residual[1, x] - (alpha[0] * i_im + alpha[1] * i_re)
            res[0, x] = re
            res[1, x] = im
            hat_re, hat_im = precondition_at(re, im, x)
            other[0, x + 2, MARGIN : MARGIN + ny, :] = hat_re
            other[1, x + 2, MARGIN : MARGIN + ny, :] = hat_im
            s_re, s_im = (shadow[0, x], shadow[1, x])
            return (acc[0] + fold(s_re * re + s_im * im), acc[1] + fold(s_re * im - s_im * re))

        acc = lax.fori_loop(0, nx, half_at, sums(2), unroll=4)
        shadow_half = (total(acc[0]), total(acc[1]))

        def second_at(x, off_re, off_im, acc):
            h_re, h_im = (res[0, x], res[1, x])
            re = h_re - off_im
            im = h_im + off_re
            second[0, x] = re
            second[1, x] = im
            s_re, s_im = (shadow[0, x], shadow[1, x])
            return (
                acc[0] + fold(re * h_re + im * h_im),
                acc[1] + fold(re * h_im - im * h_re),
                acc[2] + fold(re * re + im * im),
                acc[3] + fold(s_re * re + s_im * im),
                acc[4] + fold(s_re * im - s_im * re),
            )

        acc = over_planes(other, second_at, sums(5))
        cross_re, cross_im, norm, ss_re, ss_im = [total(part) for part in acc]
        omega = (cross_re / norm, cross_im / norm)
        alpha_hat = (alpha[0] * (1.0 / K2), alpha[1] * (1.0 / K2))
        omega_hat = (omega[0] * (1.0 / K2), omega[1] * (1.0 / K2))

        def step_evolved(base, at_d, at_h):
            along_d = complex_mul(alpha_hat, at_d)
            along_h = complex_mul(omega_hat, at_h)
            return (base[0] + (along_d[0] + along_h[0]), base[1] + (along_d[1] + along_h[1]))

        if iteration + 1 < ITERS:
            moved = complex_mul(omega, (ss_re, ss_im))
            rho_next = (shadow_half[0] - moved[0], shadow_half[1] - moved[1])
            beta = complex_mul(divide_complex(rho_next, rho), divide_complex(alpha, omega))
            beta_omega = complex_mul(beta, omega)
            rho = rho_next

            def update_at(x, carry):
                at_d = (hat[0, x + 2, MARGIN : MARGIN + ny, :], hat[1, x + 2, MARGIN : MARGIN + ny, :])
                at_h = (other[0, x + 2, MARGIN : MARGIN + ny, :], other[1, x + 2, MARGIN : MARGIN + ny, :])
                e = step_evolved((evolved[0, x], evolved[1, x]), at_d, at_h)
                evolved[0, x] = e[0]
                evolved[1, x] = e[1]
                w = complex_mul(omega, (second[0, x], second[1, x]))
                r_re = res[0, x] - w[0]
                r_im = res[1, x] - w[1]
                res[0, x] = r_re
                res[1, x] = r_im
                p = complex_mul(beta, (direction[0, x], direction[1, x]))
                v = complex_mul(beta_omega, (image[0, x], image[1, x]))
                p_re = r_re + (p[0] - v[0])
                p_im = r_im + (p[1] - v[1])
                direc[0, x] = p_re
                direc[1, x] = p_im
                hat_re, hat_im = precondition_at(p_re, p_im, x)
                hat[0, x + 2, MARGIN : MARGIN + ny, :] = hat_re
                hat[1, x + 2, MARGIN : MARGIN + ny, :] = hat_im
                return carry

            lax.fori_loop(0, nx, update_at, 0, unroll=4)
            residual, direction = (res, direc)
        else:
            own = lax.axis_index("gx") * layout.columns + lax.axis_index("gyz")
            targets = [own] + [
                layout.looked_up({(m[0], m[1]): m[2][0] * layout.columns + m[2][1] for m in r}) for r in rounds
            ]
            for target, out in zip(targets, outs):
                x0 = target // layout.columns * bx
                y0 = pl.multiple_of(lax.rem(target, layout.columns) * by, 8)

                def finish_at(i, carry):
                    x, y = (x0 + i, pl.ds(y0, by))
                    yp = pl.ds(y0 + MARGIN, by)
                    at_d = (hat[0, x + 2, yp, :], hat[1, x + 2, yp, :])
                    at_h = (other[0, x + 2, yp, :], other[1, x + 2, yp, :])
                    e = step_evolved((evolved[0, x, y, :], evolved[1, x, y, :]), at_d, at_h)
                    w = complex_mul(omega, (second[0, x, y, :], second[1, x, y, :]))
                    out[0, i] = e[0]
                    out[1, i] = e[1]
                    out[2, i] = res[0, x, y, :] - w[0]
                    out[3, i] = res[1, x, y, :] - w[1]
                    return carry

                @pl.when(target >= 0)
                def _():
                    lax.fori_loop(0, bx, finish_at, 0, unroll=4)


def unpack_kernel(layout, *refs):
    rounds = layout.deliveries()
    blocks, (evolved_ref, residual_ref) = (refs[: 1 + len(rounds)], refs[1 + len(rounds) :])
    mine = layout.solved_by(layout.here())
    orbitals = [jnp.where(mine < layout.count, mine, -1)]
    orbitals += [layout.looked_up({(m[0], m[2]): m[3] for m in r}) for r in rounds]
    for q, block in zip(orbitals, blocks):

        @pl.when(q >= 0)
        def _():
            for part in range(2):
                evolved_ref[part, q] = block[part]
                residual_ref[part, q] = block[2 + part]


VMEM_SPEC = pl.BlockSpec(memory_space=pltpu.VMEM)


def whole_call(kernel, operands, out_shapes, limit, scratch=()):
    return pl.pallas_call(
        kernel,
        out_shape=[jax.ShapeDtypeStruct(dims, jnp.float32) for dims in out_shapes],
        in_specs=[VMEM_SPEC] * len(operands),
        out_specs=[VMEM_SPEC] * len(out_shapes),
        scratch_shapes=list(scratch),
        compiler_params=pltpu.CompilerParams(vmem_limit_bytes=limit),
    )(*operands)


def solve_scratch(nx, ny, nz):
    field = pltpu.VMEM((2, nx, ny, nz), jnp.float32)
    padded = pltpu.VMEM((2, nx + 4, ny + 2 * MARGIN, nz), jnp.float32)
    scalar_field = pltpu.VMEM((nx, ny, nz), jnp.float32)
    return [scalar_field] * 2 + [padded] * 2 + [field] * 6


def gathered(layout, orbitals, potential):
    _, _, bx, by, nz = orbitals.shape
    axes = ("orb", "gx", "gyz")
    near, far, across = (layout.near, layout.far, layout.across)
    slots = 2 + layout.segments

    def fetch(array, offset, to_owner):
        return lax.ppermute(array, axes, layout.pairs(offset, to_owner))

    pots = [fetch(potential, offset, False) for offset in across]
    far_messages = whole_call(
        functools.partial(pack_far_kernel, layout), [orbitals], [(2, bx, by, nz)] * len(far), 4 * 2**20
    )
    far_blocks = [fetch(message, offset, True) for offset, message in zip(far, far_messages)]
    near_messages = whole_call(
        functools.partial(pack_near_kernel, layout),
        [orbitals, potential] + pots,
        [(slots, bx, by, nz)] * (len(near) - 1),
        4 * 2**20,
    )
    near_blocks = [fetch(message, offset, True) for offset, message in zip(near[1:], near_messages)]
    rounds = layout.deliveries()
    pieces = whole_call(
        functools.partial(solve_kernel, layout),
        [orbitals, potential] + pots + near_blocks + far_blocks,
        [(4, bx, by, nz)] * (1 + len(rounds)),
        28 * 2**20,
        solve_scratch(bx * layout.rows, by * layout.columns, nz),
    )
    arrived = [pieces[0]]
    for messages, piece in zip(rounds, pieces[1:]):
        pairs = [
            ((g * layout.rows + s[0]) * layout.columns + s[1], (g * layout.rows + d[0]) * layout.columns + d[1])
            for g in range(layout.groups)
            for parity, s, d, _ in messages
            if g % 2 == parity
        ]
        arrived.append(lax.ppermute(piece, axes, pairs))
    return whole_call(functools.partial(unpack_kernel, layout), arrived, [orbitals.shape] * 2, 6 * 2**20)


def solution(mesh):
    sizes = dict(mesh.shape)

    def shards(orbitals, potential):
        _, count, bx, by, nz = orbitals.shape
        layout = Layout(sizes["orb"], sizes["gx"], sizes["gyz"], count)
        nx, ny = (bx * layout.rows, by * layout.columns)
        fields = 24 * 4 * (nx + 4) * (ny + 2 * MARGIN) * nz
        if layout.fits and fields <= WORKING_SET and by % 8 == 0 and nz % 128 == 0:
            return tuple(gathered(layout, orbitals, potential))
        return distributed(orbitals, potential)

    return jax.shard_map(
        shards,
        mesh=mesh,
        in_specs=(P(None, "orb", "gx", "gyz", None), P("gx", "gyz", None)),
        out_specs=(P(None, "orb", "gx", "gyz", None), P(None, "orb", "gx", "gyz", None)),
        check_vma=False,
    )
```

```python
import functools
import math

import jax
import jax.numpy as jnp
from jax import lax
from jax.experimental import pallas as pl
from jax.experimental.pallas import tpu as pltpu
from jax.sharding import PartitionSpec as P


ITERS = 4


SPACING = 0.25
HALF_STEP = 0.05
COEFF_NEAR = 4.0 / 3.0
COEFF_FAR = -1.0 / 12.0
COEFF_SELF = -2.5

RATIO = -COEFF_NEAR / COEFF_FAR
K2 = HALF_STEP * -0.5 / SPACING**2 * COEFF_FAR
DIAGONAL = -0.5 / SPACING**2 * 3.0 * COEFF_SELF
MARGIN = 8
PLANES = 32
WORKING_SET = 40 * 2**20


def with_halo(array, sides, width):
    for axis, dim in sides:
        size, length = (lax.axis_size(axis), array.shape[dim])
        up = [(i, (i + 1) % size) for i in range(size - 1)]
        down = [(j, i) for i, j in up]
        last = lax.slice_in_dim(array, length - width, length, axis=dim)
        leading = lax.slice_in_dim(array, 0, width, axis=dim)
        before = lax.ppermute(last, axis, up)
        after = lax.ppermute(leading, axis, down)
        array = jnp.concatenate([before, array, after], axis=dim)
    return array


def laplace_apply(padded, potential):
    extent = (padded.shape[2] - 4, padded.shape[3] - 4, padded.shape[4] - 4)

    def window(shift_x, shift_y, shift_z):
        return padded[
            :,
            :,
            2 + shift_x : 2 + shift_x + extent[0],
            2 + shift_y : 2 + shift_y + extent[1],
            2 + shift_z : 2 + shift_z + extent[2],
        ]

    center = window(0, 0, 0)
    summed = 3.0 * COEFF_SELF * center
    for offset, weight in ((1, COEFF_NEAR), (2, COEFF_FAR)):
        summed = summed + weight * (
            window(offset, 0, 0)
            + window(-offset, 0, 0)
            + window(0, offset, 0)
            + window(0, -offset, 0)
            + window(0, 0, offset)
            + window(0, 0, -offset)
        )
    return -0.5 / SPACING**2 * summed + potential * center


def pad_depth(vector):
    return jnp.pad(vector, ((0, 0), (0, 0), (0, 0), (0, 0), (2, 2)))


def system(vector, applied):
    return jnp.stack([vector[0] - HALF_STEP * applied[1], vector[1] + HALF_STEP * applied[0]])


def precondition(vector, potential):
    diagonal = HALF_STEP * (3.75 / SPACING**2 + potential)
    divisor = 1.0 + diagonal * diagonal
    return jnp.stack(
        [(vector[0] + diagonal * vector[1]) / divisor, (vector[1] - diagonal * vector[0]) / divisor]
    )


def braket(left, right):
    real_part = jnp.sum(left[0] * right[0] + left[1] * right[1], axis=(1, 2, 3))
    imag_part = jnp.sum(left[0] * right[1] - left[1] * right[0], axis=(1, 2, 3))
    return (real_part, imag_part)


def times_complex(first, second):
    return (
        first[0] * second[0] - first[1] * second[1],
        first[0] * second[1] + first[1] * second[0],
    )


def divide_complex(first, second):
    modulus = second[0] * second[0] + second[1] * second[1]
    return (
        (first[0] * second[0] + first[1] * second[1]) / modulus,
        (first[1] * second[0] - first[0] * second[1]) / modulus,
    )


def scale_complex(coeff, vector):
    real_coef = coeff[0][:, None, None, None]
    imag_coef = coeff[1][:, None, None, None]
    return jnp.stack(
        [
            real_coef * vector[0] - imag_coef * vector[1],
            real_coef * vector[1] + imag_coef * vector[0],
        ]
    )


def distributed(orbitals, potential):
    def apply_shallow(vector):
        padded = with_halo(vector, (("gx", 2), ("gyz", 3)), 2)
        return laplace_apply(pad_depth(padded), potential)

    h_orbitals = apply_shallow(orbitals)
    residual = jnp.stack([2.0 * HALF_STEP * h_orbitals[1], -2.0 * HALF_STEP * h_orbitals[0]])
    evolved = orbitals
    shadow = residual
    direction = residual
    rho_now = lax.psum(braket(shadow, residual), ("gx", "gyz"))
    for iteration in range(ITERS):
        dir_hat = precondition(direction, potential)
        image = system(dir_hat, apply_shallow(dir_hat))
        alpha_step = divide_complex(rho_now, lax.psum(braket(shadow, image), ("gx", "gyz")))
        half_step = residual - scale_complex(alpha_step, image)
        half_hat = precondition(half_step, potential)
        second = system(half_hat, apply_shallow(half_hat))
        cross_local = braket(second, half_step)
        norm_local = jnp.sum(second * second, axis=(0, 2, 3, 4))
        shadow_half = braket(shadow, half_step)
        shadow_second = braket(shadow, second)
        summed = lax.psum(
            (
                cross_local[0],
                cross_local[1],
                norm_local,
                shadow_half[0],
                shadow_half[1],
                shadow_second[0],
                shadow_second[1],
            ),
            ("gx", "gyz"),
        )
        cross_real, cross_imag, norm_second = (summed[0], summed[1], summed[2])
        omega_step = (cross_real / norm_second, cross_imag / norm_second)
        evolved = evolved + scale_complex(alpha_step, dir_hat) + scale_complex(omega_step, half_hat)
        residual = half_step - scale_complex(omega_step, second)
        if iteration + 1 < ITERS:
            along_second = times_complex(omega_step, (summed[5], summed[6]))
            rho_next = (summed[3] - along_second[0], summed[4] - along_second[1])
            beta_step = times_complex(
                divide_complex(rho_next, rho_now), divide_complex(alpha_step, omega_step)
            )
            direction = residual + scale_complex(
                beta_step, direction - scale_complex(omega_step, image)
            )
            rho_now = rho_next
    return (evolved, residual)


class Layout:
    def __init__(self, groups, rows, columns, count):
        self.groups, self.rows, self.columns, self.count = groups, rows, columns, count
        self.width = -(-count // rows)
        self.segments = columns // self.width
        self.fits = columns % self.width == 0
        inner = [(da, dc) for da in range(rows) for dc in range(self.width)]
        self.near = [(da, 0, dc) for da, dc in inner]
        self.far = [(da, ds, dc) for ds in range(1, self.segments) for da, dc in inner]
        self.across = [(0, ds, 0) for ds in range(1, self.segments)]

    def here(self):
        b = lax.axis_index("gyz")
        return lax.axis_index("gx"), b // self.width, lax.rem(b, self.width)

    def solved_by(self, place):
        q = self.solves(place)
        return jnp.where(lax.rem(lax.axis_index("orb"), 2) == 0, q, self.rows * self.width - 1 - q)

    def moved(self, place, offset, sign=1):
        sizes = (self.rows, self.segments, self.width)
        return tuple(
            p if o == 0 else lax.rem(p + (o if sign > 0 else n - o), n)
            for p, o, n in zip(place, offset, sizes)
        )

    def solves(self, place):
        row = place[0] + place[1]
        row = row % self.rows if isinstance(row, int) else lax.rem(row, self.rows)
        return row * self.width + place[2]

    def owned(self, group, place):
        q = self.solves(place)
        return q if group % 2 == 0 else self.rows * self.width - 1 - q

    def deliveries(self):
        places = [(a, b) for a in range(self.rows) for b in range(self.columns)]
        classes = {}
        for parity in range(2):
            owner = {p: self.owned(parity, (p[0], p[1] // self.width, p[1] % self.width)) for p in places}
            for target in places:
                for q in range(self.count):
                    if owner[target] == q:
                        continue
                    hops = lambda p: abs(p[0] - target[0]) + abs(p[1] - target[1])
                    source = min((p for p in places if owner[p] == q), key=hops)
                    swap = min(target[1], source[1]) % 2 if target[0] == source[0] else 0
                    step = (target[0] != source[0], abs(target[1] - source[1]), swap)
                    classes.setdefault(step, []).append((parity, source, target, q))
        rounds = []
        for step in sorted(classes, key=lambda s: (s[2], s[0], -s[1])):
            for r in rounds:
                busy = {(m[0], m[1], 0) for m in r} | {(m[0], m[2], 1) for m in r}
                if not any((m[0], m[1], 0) in busy or (m[0], m[2], 1) in busy for m in classes[step]):
                    r += classes[step]
                    break
            else:
                rounds.append(list(classes[step]))
        return rounds

    def looked_up(self, entries):
        parity = lax.rem(lax.axis_index("orb"), 2)
        index = (parity * self.rows + lax.axis_index("gx")) * self.columns + lax.axis_index("gyz")
        value = jnp.int32(-1)
        for (p, (a, b)), entry in entries.items():
            value = jnp.where(index == (p * self.rows + a) * self.columns + b, entry, value)
        return value

    def pairs(self, offset, to_owner):
        found = []
        for g in range(self.groups):
            for a in range(self.rows):
                for b in range(self.columns):
                    place = (a, b // self.width, b % self.width)
                    sizes = (self.rows, self.segments, self.width)
                    other = tuple((p + o) % n for p, o, n in zip(place, offset, sizes))
                    source, target = (other, place)
                    if not to_owner or self.owned(g, target) < self.count:
                        found.append((self.linear(g, source), self.linear(g, target)))
        return found

    def linear(self, g, place):
        return (g * self.rows + place[0]) * self.columns + place[1] * self.width + place[2]


def complex_mul(first, second):
    return (
        first[0] * second[0] - first[1] * second[1],
        first[0] * second[1] + first[1] * second[0],
    )


def pack_far_kernel(layout, orbitals_ref, *out_refs):
    here = layout.here()
    for offset, out_ref in zip(layout.far, out_refs):
        q = jnp.minimum(layout.solved_by(layout.moved(here, offset, -1)), layout.count - 1)
        out_ref[0] = orbitals_ref[0, q]
        out_ref[1] = orbitals_ref[1, q]


def pack_near_kernel(layout, orbitals_ref, potential_ref, *refs):
    others, out_refs = (refs[: len(layout.across)], refs[len(layout.across) :])
    here = layout.here()
    for offset, out_ref in zip(layout.near[1:], out_refs):
        q = jnp.minimum(layout.solved_by(layout.moved(here, offset, -1)), layout.count - 1)
        out_ref[0] = orbitals_ref[0, q]
        out_ref[1] = orbitals_ref[1, q]
        for slot, ref in enumerate((potential_ref,) + tuple(others)):
            out_ref[2 + slot] = ref[...]


def total(parts):
    return jnp.sum(jnp.sum(parts, axis=0, keepdims=True), axis=1, keepdims=True)


def fold(product):
    return jnp.sum(product.reshape(-1, 8, product.shape[-1]), axis=0)


def solve_kernel(layout, *refs):
    near, far, across = (layout.near, layout.far, layout.across)
    orbitals_ref, potential_ref = refs[:2]
    refs = refs[2:]
    pots, refs = (refs[: len(across)], refs[len(across) :])
    near_refs, refs = (refs[: len(near) - 1], refs[len(near) - 1 :])
    far_refs, refs = (refs[: len(far)], refs[len(far) :])
    rounds = layout.deliveries()
    outs, scratch = (refs[: 1 + len(rounds)], refs[1 + len(rounds) :])
    diag, inv, padded_d, padded_h, evolved, res, shadow, direc, image, second = scratch
    bx, by, nz = potential_ref.shape
    nx, ny = (bx * layout.rows, by * layout.columns)
    planes = math.gcd(nx, PLANES)
    here = layout.here()

    def corner(offset):
        a, s, c = layout.moved(here, offset)
        return a * bx, pl.multiple_of((s * layout.width + c) * by, 8)

    zero_edge = jnp.zeros((2, 2, ny + 2 * MARGIN, nz), jnp.float32)
    for padded in (padded_d, padded_h):
        padded[:, 0:2] = zero_edge
        padded[:, nx + 2 : nx + 4] = zero_edge
        padded[:, :, 0:MARGIN] = jnp.zeros((2, nx + 4, MARGIN, nz), jnp.float32)
        padded[:, :, ny + MARGIN : ny + 2 * MARGIN] = jnp.zeros((2, nx + 4, MARGIN, nz), jnp.float32)

    def place_orbital(offset, part, block):
        x0, y0 = corner(offset)
        padded_d[part, pl.ds(x0 + 2, bx), pl.ds(y0 + MARGIN, by), :] = block
        evolved[part, pl.ds(x0, bx), pl.ds(y0, by), :] = block

    def place_potential(offset, block):
        x0, y0 = corner(offset)
        d = HALF_STEP * (DIAGONAL + block)
        diag[pl.ds(x0, bx), pl.ds(y0, by), :] = d
        inv[pl.ds(x0, bx), pl.ds(y0, by), :] = K2 / (1.0 + d * d)

    mine = jnp.minimum(layout.solved_by(here), layout.count - 1)
    place_potential(near[0], potential_ref[...])
    for offset, ref in zip(across, pots):
        place_potential(offset, ref[...])
    for part in range(2):
        place_orbital(near[0], part, orbitals_ref[part, mine])
    for (da, _, dc), ref in zip(near[1:], near_refs):
        for ds in range(layout.segments):
            place_potential((da, ds, dc), ref[2 + ds])
        for part in range(2):
            place_orbital((da, 0, dc), part, ref[part])
    for offset, ref in zip(far, far_refs):
        for part in range(2):
            place_orbital(offset, part, ref[part])

    apart = jnp.abs(lax.broadcasted_iota(jnp.int32, (2 * nz, nz), 0) % nz - lax.broadcasted_iota(jnp.int32, (2 * nz, nz), 1))
    weights = jnp.where(apart == 1, -RATIO, jnp.where(apart == 2, 1.0, 0.0)).astype(jnp.bfloat16)

    def along_z(center):
        high = center.astype(jnp.bfloat16)
        low = (center - high.astype(jnp.float32)).astype(jnp.bfloat16)
        return jnp.dot(jnp.concatenate([high, low], axis=1), weights, preferred_element_type=jnp.float32)

    def stencils(padded, x):
        rows = pl.ds(MARGIN, ny)
        flat = [padded[part, pl.ds(x + 2, planes), rows, :].reshape(planes * ny, nz) for part in range(2)]
        deep = along_z(jnp.concatenate(flat, axis=0))

        def at(part, i):
            def ring(s):
                return (padded[part, x + i + 2 + s, rows, :] + padded[part, x + i + 2 - s, rows, :]) + (
                    padded[part, x + i + 2, MARGIN + s : MARGIN + s + ny, :]
                    + padded[part, x + i + 2, MARGIN - s : MARGIN - s + ny, :]
                )

            start = (part * planes + i) * ny
            return (ring(2) - RATIO * ring(1)) + deep[start : start + ny]

        return [[at(part, i) for i in range(planes)] for part in range(2)]

    def over_planes(padded, at, acc):
        def step(i, acc):
            base = i * planes
            re, im = stencils(padded, base)
            for k in range(planes):
                acc = at(base + k, re[k], im[k], acc)
            return acc

        return lax.fori_loop(0, nx // planes, step, acc)

    def sums(count):
        return tuple(jnp.zeros((8, nz), jnp.float32) for _ in range(count))

    def precondition_at(re, im, x):
        d, scale = (diag[x], inv[x])
        return (re + d * im) * scale, (im - d * re) * scale

    def start(x, off_re, off_im, acc):
        d = diag[x]
        center_re = padded_d[0, x + 2, MARGIN : MARGIN + ny, :]
        center_im = padded_d[1, x + 2, MARGIN : MARGIN + ny, :]
        re = 2.0 * (d * center_im + K2 * off_im)
        im = -2.0 * (d * center_re + K2 * off_re)
        shadow[0, x] = re
        shadow[1, x] = im
        hat_re, hat_im = precondition_at(re, im, x)
        padded_h[0, x + 2, MARGIN : MARGIN + ny, :] = hat_re
        padded_h[1, x + 2, MARGIN : MARGIN + ny, :] = hat_im
        return (acc[0] + fold(re * re + im * im),)

    (norm,) = over_planes(padded_d, start, sums(1))
    rho = (total(norm), jnp.zeros((1, 1), jnp.float32))
    residual, direction = (shadow, shadow)
    hat, other = (padded_h, padded_d)

    for iteration in range(ITERS):

        def image_at(x, off_re, off_im, acc):
            re = direction[0, x] - off_im
            im = direction[1, x] + off_re
            image[0, x] = re
            image[1, x] = im
            s_re, s_im = (shadow[0, x], shadow[1, x])
            return (acc[0] + fold(s_re * re + s_im * im), acc[1] + fold(s_re * im - s_im * re))

        acc = over_planes(hat, image_at, sums(2))
        sigma = (total(acc[0]), total(acc[1]))
        alpha = divide_complex(rho, sigma)

        def half_at(x, acc):
            i_re, i_im = (image[0, x], image[1, x])
            re = residual[0, x] - (alpha[0] * i_re - alpha[1] * i_im)
            im = residual[1, x] - (alpha[0] * i_im + alpha[1] * i_re)
            res[0, x] = re
            res[1, x] = im
            hat_re, hat_im = precondition_at(re, im, x)
            other[0, x + 2, MARGIN : MARGIN + ny, :] = hat_re
            other[1, x + 2, MARGIN : MARGIN + ny, :] = hat_im
            s_re, s_im = (shadow[0, x], shadow[1, x])
            return (acc[0] + fold(s_re * re + s_im * im), acc[1] + fold(s_re * im - s_im * re))

        acc = lax.fori_loop(0, nx, half_at, sums(2), unroll=8)
        shadow_half = (total(acc[0]), total(acc[1]))

        def second_at(x, off_re, off_im, acc):
            h_re, h_im = (res[0, x], res[1, x])
            re = h_re - off_im
            im = h_im + off_re
            second[0, x] = re
            second[1, x] = im
            s_re, s_im = (shadow[0, x], shadow[1, x])
            return (
                acc[0] + fold(re * h_re + im * h_im),
                acc[1] + fold(re * h_im - im * h_re),
                acc[2] + fold(re * re + im * im),
                acc[3] + fold(s_re * re + s_im * im),
                acc[4] + fold(s_re * im - s_im * re),
            )

        acc = over_planes(other, second_at, sums(5))
        cross_re, cross_im, norm, ss_re, ss_im = [total(part) for part in acc]
        omega = (cross_re / norm, cross_im / norm)
        alpha_hat = (alpha[0] * (1.0 / K2), alpha[1] * (1.0 / K2))
        omega_hat = (omega[0] * (1.0 / K2), omega[1] * (1.0 / K2))

        def step_evolved(base, at_d, at_h):
            along_d = complex_mul(alpha_hat, at_d)
            along_h = complex_mul(omega_hat, at_h)
            return (base[0] + (along_d[0] + along_h[0]), base[1] + (along_d[1] + along_h[1]))

        if iteration + 1 < ITERS:
            moved = complex_mul(omega, (ss_re, ss_im))
            rho_next = (shadow_half[0] - moved[0], shadow_half[1] - moved[1])
            beta = complex_mul(divide_complex(rho_next, rho), divide_complex(alpha, omega))
            beta_omega = complex_mul(beta, omega)
            rho = rho_next

            def update_at(x, carry):
                at_d = (hat[0, x + 2, MARGIN : MARGIN + ny, :], hat[1, x + 2, MARGIN : MARGIN + ny, :])
                at_h = (other[0, x + 2, MARGIN : MARGIN + ny, :], other[1, x + 2, MARGIN : MARGIN + ny, :])
                e = step_evolved((evolved[0, x], evolved[1, x]), at_d, at_h)
                evolved[0, x] = e[0]
                evolved[1, x] = e[1]
                w = complex_mul(omega, (second[0, x], second[1, x]))
                r_re = res[0, x] - w[0]
                r_im = res[1, x] - w[1]
                res[0, x] = r_re
                res[1, x] = r_im
                p = complex_mul(beta, (direction[0, x], direction[1, x]))
                v = complex_mul(beta_omega, (image[0, x], image[1, x]))
                p_re = r_re + (p[0] - v[0])
                p_im = r_im + (p[1] - v[1])
                direc[0, x] = p_re
                direc[1, x] = p_im
                hat_re, hat_im = precondition_at(p_re, p_im, x)
                hat[0, x + 2, MARGIN : MARGIN + ny, :] = hat_re
                hat[1, x + 2, MARGIN : MARGIN + ny, :] = hat_im
                return carry

            lax.fori_loop(0, nx, update_at, 0, unroll=8)
            residual, direction = (res, direc)
        else:
            own = lax.axis_index("gx") * layout.columns + lax.axis_index("gyz")
            targets = [own] + [
                layout.looked_up({(m[0], m[1]): m[2][0] * layout.columns + m[2][1] for m in r}) for r in rounds
            ]
            for target, out in zip(targets, outs):
                x0 = target // layout.columns * bx
                y0 = pl.multiple_of(lax.rem(target, layout.columns) * by, 8)

                def finish_at(i, carry):
                    x, y = (x0 + i, pl.ds(y0, by))
                    yp = pl.ds(y0 + MARGIN, by)
                    at_d = (hat[0, x + 2, yp, :], hat[1, x + 2, yp, :])
                    at_h = (other[0, x + 2, yp, :], other[1, x + 2, yp, :])
                    e = step_evolved((evolved[0, x, y, :], evolved[1, x, y, :]), at_d, at_h)
                    w = complex_mul(omega, (second[0, x, y, :], second[1, x, y, :]))
                    out[0, i] = e[0]
                    out[1, i] = e[1]
                    out[2, i] = res[0, x, y, :] - w[0]
                    out[3, i] = res[1, x, y, :] - w[1]
                    return carry

                @pl.when(target >= 0)
                def _():
                    lax.fori_loop(0, bx, finish_at, 0, unroll=8)


def unpack_kernel(layout, *refs):
    rounds = layout.deliveries()
    blocks, (evolved_ref, residual_ref) = (refs[: 1 + len(rounds)], refs[1 + len(rounds) :])
    mine = layout.solved_by(layout.here())
    orbitals = [jnp.where(mine < layout.count, mine, -1)]
    orbitals += [layout.looked_up({(m[0], m[2]): m[3] for m in r}) for r in rounds]
    for q, block in zip(orbitals, blocks):

        @pl.when(q >= 0)
        def _():
            for part in range(2):
                evolved_ref[part, q] = block[part]
                residual_ref[part, q] = block[2 + part]


VMEM_SPEC = pl.BlockSpec(memory_space=pltpu.VMEM)


def whole_call(kernel, operands, out_shapes, limit, scratch=()):
    return pl.pallas_call(
        kernel,
        out_shape=[jax.ShapeDtypeStruct(dims, jnp.float32) for dims in out_shapes],
        in_specs=[VMEM_SPEC] * len(operands),
        out_specs=[VMEM_SPEC] * len(out_shapes),
        scratch_shapes=list(scratch),
        compiler_params=pltpu.CompilerParams(vmem_limit_bytes=limit),
    )(*operands)


def solve_scratch(nx, ny, nz):
    field = pltpu.VMEM((2, nx, ny, nz), jnp.float32)
    padded = pltpu.VMEM((2, nx + 4, ny + 2 * MARGIN, nz), jnp.float32)
    scalar_field = pltpu.VMEM((nx, ny, nz), jnp.float32)
    return [scalar_field] * 2 + [padded] * 2 + [field] * 6


def gathered(layout, orbitals, potential):
    _, _, bx, by, nz = orbitals.shape
    axes = ("orb", "gx", "gyz")
    near, far, across = (layout.near, layout.far, layout.across)
    slots = 2 + layout.segments

    def fetch(array, offset, to_owner):
        return lax.ppermute(array, axes, layout.pairs(offset, to_owner))

    pots = [fetch(potential, offset, False) for offset in across]
    far_messages = whole_call(
        functools.partial(pack_far_kernel, layout), [orbitals], [(2, bx, by, nz)] * len(far), 4 * 2**20
    )
    far_blocks = [fetch(message, offset, True) for offset, message in zip(far, far_messages)]
    near_messages = whole_call(
        functools.partial(pack_near_kernel, layout),
        [orbitals, potential] + pots,
        [(slots, bx, by, nz)] * (len(near) - 1),
        4 * 2**20,
    )
    near_blocks = [fetch(message, offset, True) for offset, message in zip(near[1:], near_messages)]
    rounds = layout.deliveries()
    pieces = whole_call(
        functools.partial(solve_kernel, layout),
        [orbitals, potential] + pots + near_blocks + far_blocks,
        [(4, bx, by, nz)] * (1 + len(rounds)),
        28 * 2**20,
        solve_scratch(bx * layout.rows, by * layout.columns, nz),
    )
    arrived = [pieces[0]]
    for messages, piece in zip(rounds, pieces[1:]):
        pairs = [
            ((g * layout.rows + s[0]) * layout.columns + s[1], (g * layout.rows + d[0]) * layout.columns + d[1])
            for g in range(layout.groups)
            for parity, s, d, _ in messages
            if g % 2 == parity
        ]
        arrived.append(lax.ppermute(piece, axes, pairs))
    return whole_call(functools.partial(unpack_kernel, layout), arrived, [orbitals.shape] * 2, 6 * 2**20)


def solution(mesh):
    sizes = dict(mesh.shape)

    def shards(orbitals, potential):
        _, count, bx, by, nz = orbitals.shape
        layout = Layout(sizes["orb"], sizes["gx"], sizes["gyz"], count)
        nx, ny = (bx * layout.rows, by * layout.columns)
        fields = 24 * 4 * (nx + 4) * (ny + 2 * MARGIN) * nz
        if layout.fits and fields <= WORKING_SET and by % 8 == 0 and nz % 128 == 0:
            return tuple(gathered(layout, orbitals, potential))
        return distributed(orbitals, potential)

    return jax.shard_map(
        shards,
        mesh=mesh,
        in_specs=(P(None, "orb", "gx", "gyz", None), P("gx", "gyz", None)),
        out_specs=(P(None, "orb", "gx", "gyz", None), P(None, "orb", "gx", "gyz", None)),
        check_vma=False,
    )
```
